16 devices in a mesh: data: 2 (over y, z), seq: 8 (over x, core).
Axes of the slice: x: 4, y: 2, z: 1, core: 2. Of those that a mesh axis runs over, the one named last changes fastest.
The devices are a block of a 4x4x8 slice.
Arguments:
- tokens: bfloat16 [4, 512, 1024], P('data', 'seq'), parts along dimension 0
- lengths: int32 [4], P('data'), parts along dimension 0
- slot_param: bfloat16 [1024, 1024], replicated
- logit_scale: float32 [], replicated
- w_in: bfloat16 [64, 1024, 4096], P('seq')
- w_out: bfloat16 [64, 4096, 1024], P('seq')
Outputs:
- output: bfloat16 [4, 512, 1024], P('data', 'seq'), parts along dimension 0
There are 2 independent parts. The reference program is written for one: setup_inputs(seed, part) draws one part's arguments, and reference() takes and returns one part's arrays. A program takes and returns all parts, laid end to end along the dimension named above; an argument that names none is the same for every part.
All inputs are finite; a program needn't handle non-finite values.
Results may differ from the reference program's by a relative error of at most 0.013898.
Values are sent between devices in bfloat16 or wider.
A program may use at most 768 MiB of HBM per device.

```python
import jax
import jax.numpy as jnp
from jax import lax

BATCH = 2
TOKENS = 512
D_MODEL = 1024
FF_DIM = 4096
EXPERTS = 64
SLOTS = 16
LATENT = 16

N_SLOTS = EXPERTS * SLOTS
EPSILON = 1e-6
NEG_FILL = -1e30


def setup_inputs(seed: int = 0, part: int = 0) -> dict:
    shared = jax.random.split(jax.random.key(seed), 6)
    own = jax.random.split(jax.random.fold_in(jax.random.key(seed + 1), part), 3)
    basis = jax.random.normal(shared[0], (LATENT, D_MODEL), jnp.float32)
    phi_code = jax.random.normal(shared[1], (LATENT, N_SLOTS), jnp.float32)
    slot_param = jnp.dot(basis.T, phi_code) / LATENT ** 0.5 + 0.5 * jax.random.normal(shared[2], (D_MODEL, N_SLOTS), jnp.float32)
    logit_scale = 6.0 + 4.0 * jax.random.uniform(shared[3], (), jnp.float32)
    w_in = 2.0 * D_MODEL ** -0.5 * jax.random.normal(shared[4], (EXPERTS, D_MODEL, FF_DIM), jnp.float32)
    w_out = 2.0 * FF_DIM ** -0.5 * jax.random.normal(shared[5], (EXPERTS, FF_DIM, D_MODEL), jnp.float32)
    tok_code = jax.random.normal(own[0], (BATCH, TOKENS, LATENT), jnp.float32)
    tokens = jnp.einsum("btl,ld->btd", tok_code, basis) / LATENT ** 0.5 + 0.5 * jax.random.normal(own[1], (BATCH, TOKENS, D_MODEL), jnp.float32)
    drawn = jax.random.randint(own[2], (BATCH,), 1, TOKENS + 1, jnp.int32)
    lengths = jnp.where(jnp.arange(BATCH) == 0, TOKENS, drawn).astype(jnp.int32)
    return {"tokens": tokens.astype(jnp.bfloat16), "lengths": lengths, "slot_param": slot_param.astype(jnp.bfloat16), "logit_scale": logit_scale, "w_in": w_in.astype(jnp.bfloat16), "w_out": w_out.astype(jnp.bfloat16)}


def l2_normed(values, axis_dim):
    v32 = values.astype(jnp.float32)
    return (v32 * lax.rsqrt(jnp.sum(v32 * v32, axis=axis_dim, keepdims=True) + EPSILON)).astype(jnp.bfloat16)


def reference(tokens, lengths, slot_param, logit_scale, w_in, w_out):
    phi_norm = l2_normed(slot_param, 0).astype(jnp.float32)
    positions = jnp.arange(TOKENS, dtype=jnp.int32)

    def row_logits(tok_row):
        tok_norm = l2_normed(tok_row, 1).astype(jnp.float32)
        return logit_scale * jnp.dot(tok_norm, phi_norm, preferred_element_type=jnp.float32)

    def dispatch_row(row_args):
        tok_row, len_row = row_args
        logits = row_logits(tok_row)
        masked = jnp.where((positions < len_row)[:, None], logits, NEG_FILL)
        disp_w = jnp.exp(masked - jnp.max(masked, axis=0, keepdims=True))
        col_sum = jnp.sum(disp_w, axis=0)
        slot_sum = jnp.dot(disp_w.astype(jnp.bfloat16).astype(jnp.float32).T, tok_row.astype(jnp.float32), preferred_element_type=jnp.float32)
        return (slot_sum / col_sum[:, None]).astype(jnp.bfloat16)

    slot_in = lax.map(dispatch_row, (tokens, lengths))
    slot_grp = jnp.transpose(slot_in.reshape(BATCH, EXPERTS, SLOTS, D_MODEL), (1, 0, 2, 3))

    def expert_ffn(exp_args):
        slot_exp, win_exp, wout_exp = exp_args
        hidden = jnp.einsum("bsd,df->bsf", slot_exp.astype(jnp.float32), win_exp.astype(jnp.float32))
        hidden = jax.nn.gelu(hidden).astype(jnp.bfloat16)
        return jnp.einsum("bsf,fd->bsd", hidden.astype(jnp.float32), wout_exp.astype(jnp.float32)).astype(jnp.bfloat16)

    slot_out = lax.map(expert_ffn, (slot_grp, w_in, w_out))
    slot_out = jnp.transpose(slot_out, (1, 0, 2, 3)).reshape(BATCH, N_SLOTS, D_MODEL)

    def combine_row(row_args):
        tok_row, len_row, out_row = row_args
        logits = row_logits(tok_row)
        comb_w = jnp.exp(logits - jnp.max(logits, axis=1, keepdims=True))
        row_sum = jnp.sum(comb_w, axis=1, keepdims=True)
        tok_mixed = jnp.dot(comb_w.astype(jnp.bfloat16).astype(jnp.float32), out_row.astype(jnp.float32), preferred_element_type=jnp.float32) / row_sum
        return jnp.where((positions < len_row)[:, None], tok_mixed, 0.0).astype(jnp.bfloat16)

    return lax.map(combine_row, (tokens, lengths, slot_out))
```

```python
import functools

import jax
import jax.numpy as jnp
from jax import lax
from jax.experimental import pallas as pl
from jax.experimental.pallas import tpu as pltpu
from jax.sharding import PartitionSpec as P

EPSILON = 1e-6
NEG_FILL = -1e30
MESH = pl.DeviceIdType.MESH
F32 = jnp.float32
BF16 = jnp.bfloat16
FF_BLOCK = 1024
AHEAD = 12


def unit_rows(values):
    v32 = values.astype(F32)
    return (v32 * lax.rsqrt(jnp.sum(v32 * v32, axis=1, keepdims=True) + EPSILON)).astype(BF16)


class Exchange:
    def __init__(self, me, n, chunk, send_sem, recv_sem):
        core = lax.rem(me, 2)
        self.me, self.mate = me, me + 1 - 2 * core
        self.right, self.left = lax.rem(me + 2, n), lax.rem(me + n - 2, n)
        self.far = lax.rem(me + n // 2, n)
        self.rightm, self.leftm, self.farm = (p + 1 - 2 * core for p in (self.right, self.left, self.far))
        self.chunk, self.send_sem, self.recv_sem = chunk, send_sem, recv_sem

    def copy(self, i, half, src, to):
        ref = self.chunk(half, src)
        return pltpu.make_async_remote_copy(src_ref=ref, dst_ref=ref, send_sem=self.send_sem(i), recv_sem=self.recv_sem(half, src), device_id={"seq": to}, device_id_type=MESH)

    def plan(self):
        return [(0, self.me, self.right), (1, self.me, self.right), (1, self.me, self.left), (0, self.me, self.left), (0, self.me, self.mate), (1, self.me, self.mate),
                (0, self.left, self.right), (1, self.right, self.left), (0, self.left, self.mate), (1, self.right, self.mate),
                (1, self.left, self.mate), (0, self.right, self.mate), (0, self.far, self.mate), (1, self.far, self.mate)]

    def start(self, first, last):
        for i, (half, src, to) in list(enumerate(self.plan()))[first:last]:
            self.copy(i, half, src, to).start()

    def arrived(self, *pairs):
        for half, src in pairs:
            self.copy(0, half, src, self.mate).wait_recv()

    def own(self):
        self.start(0, 6)

    def first(self):
        self.arrived((0, self.left), (1, self.right))
        self.start(6, 10)

    def second(self):
        self.arrived((1, self.left), (0, self.right))
        self.start(10, 12)

    def third(self):
        self.arrived((0, self.far), (1, self.far))
        self.start(12, 14)

    def from_mate(self, *sources):
        for src in sources:
            self.arrived((0, src), (1, src))

    def sent(self):
        for i, (half, src, to) in enumerate(self.plan()):
            self.copy(i, half, src, to).wait_send()


def kernel(n, tok_hbm, len_ref, phi_hbm, g_ref, w1_hbm, w2_hbm, out_ref, xall, phi, pnt, lt, cbuf, qbuf, cperm, xs, ysall, yexp, yacc, w1buf, w2buf,
           loc_sem, w1_sem, w2_sem, tok_send, tok_recv, ys_send, ys_recv):
    batch, _, toks, d_model = xall.shape
    n_exp, _, rows, _ = ysall.shape
    per_exp = rows // batch
    slot_loc = n_exp * per_exp
    blocks = w1_hbm.shape[2] // FF_BLOCK
    units = n_exp * blocks
    ahead = w1buf.shape[0]
    chips = n // 2
    me = lax.axis_index("seq")
    g = g_ref[0]

    def w_copies(u):
        slot, e = lax.rem(u, ahead), u // blocks
        f0 = pl.multiple_of(lax.rem(u, blocks) * FF_BLOCK, FF_BLOCK)
        return (pltpu.make_async_copy(w1_hbm.at[e, :, pl.ds(f0, FF_BLOCK)], w1buf.at[slot], w1_sem.at[slot]),
                pltpu.make_async_copy(w2_hbm.at[e, pl.ds(f0, FF_BLOCK), :], w2buf.at[slot], w2_sem.at[slot]))

    tok_ex = Exchange(me, n, lambda half, src: xall.at[half, src], lambda i: tok_send.at[i], lambda half, src: tok_recv.at[half, src])
    barrier = pltpu.get_barrier_semaphore()
    for peer in (tok_ex.right, tok_ex.left, tok_ex.mate):
        pl.semaphore_signal(barrier, inc=1, device_id={"seq": peer}, device_id_type=MESH)
    own_in = [pltpu.make_async_copy(tok_hbm.at[b], xall.at[b, me], loc_sem.at[b]) for b in range(batch)]
    for c in own_in:
        c.start()
    phi_in = pltpu.make_async_copy(phi_hbm, phi, loc_sem.at[batch])
    phi_in.start()

    def first_weights(u, _):
        for c in w_copies(u):
            c.start()
        return 0

    lax.fori_loop(0, ahead, first_weights, 0)
    for c in own_in:
        c.wait()
    pl.semaphore_wait(barrier, 3)
    tok_ex.own()

    phi_in.wait()
    d_rows = phi.shape[0]
    n_slots = phi.shape[1]
    step = 64

    def sum_sq(i, acc):
        v = phi[pl.ds(pl.multiple_of(i * step, step), step), :].astype(F32)
        return acc + jnp.sum((v * v).reshape(step // 8, 8, n_slots), axis=0)

    scale = lax.rsqrt(jnp.sum(lax.fori_loop(0, d_rows // step, sum_sq, jnp.zeros((8, n_slots), F32)), axis=0, keepdims=True) + EPSILON)

    def to_unit(i, _):
        at = pl.ds(pl.multiple_of(i * step, step), step)
        phi[at, :] = (phi[at, :].astype(F32) * scale).astype(BF16)
        return 0

    lax.fori_loop(0, d_rows // step, to_unit, 0)
    pnt[...] = phi[:, pl.ds(pl.multiple_of(me * slot_loc, slot_loc), slot_loc)].astype(F32).T.astype(BF16)

    for b in range(batch):
        logits = g * jnp.dot(unit_rows(xall[b, me]), phi[...], preferred_element_type=F32)
        comb = jnp.exp(logits - jnp.max(logits, axis=1, keepdims=True))
        at = pl.ds(b * toks, toks)
        qbuf[at, :] = jnp.broadcast_to(jnp.sum(comb, axis=1, keepdims=True), (toks, 128))
        cbuf[at, :] = comb.astype(BF16)

    tok_ex.first()

    def per_expert(e, _):
        j = lax.broadcasted_iota(jnp.int32, (n_slots, slot_loc), 0)
        k = lax.broadcasted_iota(jnp.int32, (n_slots, slot_loc), 1)
        pick = (j == (k // per_exp) * slot_loc + e * per_exp + lax.rem(k, per_exp)).astype(F32).astype(BF16)
        cperm[e] = jnp.dot(cbuf[...], pick, preferred_element_type=F32).astype(BF16)
        return 0

    lax.fori_loop(0, n_exp, per_expert, 0)

    def chip_logits(chip):
        for b in range(batch):
            x_chip = xall[b, pl.ds(2 * chip, 2)].reshape(2 * toks, d_model)
            logits = g * lax.dot_general(pnt[...], unit_rows(x_chip), (((1,), (1,)), ((), ())), preferred_element_type=F32)
            pos = chip * (2 * toks) + lax.broadcasted_iota(jnp.int32, logits.shape, 1)
            lt[b, chip] = jnp.where(pos < len_ref[b], logits, NEG_FILL)

    tok_ex.from_mate(tok_ex.mate)
    chip_logits(me // 2)
    tok_ex.second()
    tok_ex.from_mate(tok_ex.leftm, tok_ex.rightm)
    chip_logits(tok_ex.left // 2)
    chip_logits(tok_ex.right // 2)
    tok_ex.third()
    tok_ex.from_mate(tok_ex.farm)
    chip_logits(tok_ex.far // 2)

    for b in range(batch):
        parts = [lt[b, k] for k in range(chips)]
        top = jnp.max(functools.reduce(jnp.maximum, parts), axis=1, keepdims=True)
        disp = [jnp.exp(p - top) for p in parts]
        col_sum = jnp.sum(functools.reduce(jnp.add, disp), axis=1, keepdims=True)
        weights = jnp.concatenate([w.astype(BF16) for w in disp], axis=1)
        slot_sum = jnp.dot(weights, xall[b].reshape(n * toks, d_model), preferred_element_type=F32)
        xs[:, pl.ds(b * per_exp, per_exp), :] = (slot_sum / col_sum).astype(BF16).reshape(n_exp, per_exp, d_model)
    tok_ex.sent()
    yacc[...] = jnp.zeros_like(yacc)

    def ys_ex(e):
        return Exchange(me, n, lambda half, src: ysall.at[e, src, pl.ds(half * per_exp, per_exp)], lambda i: ys_send.at[lax.rem(e, 2), i], lambda half, src: ys_recv.at[e, half, src])

    def combine(e):
        for b in range(batch):
            at = pl.ds(b * toks, toks)
            got = ysall[e, :, pl.ds(b * per_exp, per_exp), :].reshape(n * per_exp, d_model)
            yacc[at, :] += jnp.dot(cperm[e, at, :], got, preferred_element_type=F32)

    def finish(e):
        ex = ys_ex(e)
        ex.from_mate(ex.mate, ex.leftm, ex.rightm, ex.farm)
        combine(e)
        ex.sent()

    def expert(e, _):
        for j in range(blocks):
            u = e * blocks + j
            slot = lax.rem(u, ahead)
            c1, c2 = w_copies(u)
            c1.wait()
            hidden = jax.nn.gelu(jnp.dot(xs[e], w1buf[slot], preferred_element_type=F32)).astype(BF16)
            c2.wait()
            part = jnp.dot(hidden, w2buf[slot], preferred_element_type=F32)
            if j == 0:
                yexp[...] = part
            else:
                yexp[...] += part

            @pl.when(u + ahead < units)
            def _():
                for c in w_copies(u + ahead):
                    c.start()

            if j == 0:
                @pl.when(e >= 1)
                def _():
                    ys_ex(e - 1).own()
            if j == 1:
                @pl.when(e >= 2)
                def _():
                    ys_ex(e - 2).third()
            if j == 2:
                @pl.when(e >= 2)
                def _():
                    finish(e - 2)
            if j == 3:
                @pl.when(e >= 1)
                def _():
                    ys_ex(e - 1).first()
                    ys_ex(e - 1).second()
        ysall[e, me] = yexp[...].astype(BF16)
        return 0

    lax.fori_loop(0, n_exp, expert, 0)
    ys_ex(n_exp - 1).own()
    ys_ex(n_exp - 2).third()
    finish(n_exp - 2)
    ys_ex(n_exp - 1).first()
    ys_ex(n_exp - 1).second()
    ys_ex(n_exp - 1).third()
    finish(n_exp - 1)

    for b in range(batch):
        at = pl.ds(b * toks, toks)
        pos = me * toks + lax.broadcasted_iota(jnp.int32, (toks, 1), 0)
        out_ref[b] = jnp.where(pos < len_ref[b], yacc[at, :] / qbuf[at, 0:1], 0.0).astype(BF16)


def solution(mesh):
    n = mesh.shape["seq"]

    def local_layer(tok_blk, len_blk, slot_param, logit_scale, w_in, w_out):
        batch, toks, d_model = tok_blk.shape
        n_slots = slot_param.shape[1]
        n_exp = w_in.shape[0]
        slot_loc = n_slots // n
        rows = batch * (slot_loc // n_exp)
        dma = pltpu.SemaphoreType.DMA
        any_spec = pl.BlockSpec(memory_space=pl.ANY)
        smem_spec = pl.BlockSpec(memory_space=pltpu.SMEM)
        return pl.pallas_call(
            functools.partial(kernel, n),
            out_shape=jax.ShapeDtypeStruct(tok_blk.shape, BF16),
            in_specs=[any_spec, smem_spec, any_spec, smem_spec, any_spec, any_spec],
            out_specs=pl.BlockSpec(memory_space=pltpu.VMEM),
            scratch_shapes=[
                pltpu.VMEM((batch, n, toks, d_model), BF16),
                pltpu.VMEM(slot_param.shape, BF16),
                pltpu.VMEM((slot_loc, d_model), BF16),
                pltpu.VMEM((batch, n // 2, slot_loc, 2 * toks), F32),
                pltpu.VMEM((batch * toks, n_slots), BF16),
                pltpu.VMEM((batch * toks, 128), F32),
                pltpu.VMEM((n_exp, batch * toks, n_slots // n_exp), BF16),
                pltpu.VMEM((n_exp, rows, d_model), BF16),
                pltpu.VMEM((n_exp, n, rows, d_model), BF16),
                pltpu.VMEM((rows, d_model), F32),
                pltpu.VMEM((batch * toks, d_model), F32),
                pltpu.VMEM((AHEAD, d_model, FF_BLOCK), BF16),
                pltpu.VMEM((AHEAD, FF_BLOCK, d_model), BF16),
                dma((batch + 1,)), dma((AHEAD,)), dma((AHEAD,)),
                dma((14,)), dma((batch, n)), dma((2, 14)), dma((n_exp, batch, n)),
            ],
            compiler_params=pltpu.CompilerParams(collective_id=0, has_side_effects=True, vmem_limit_bytes=67043328),
        )(tok_blk, len_blk, slot_param, logit_scale.reshape(1), w_in, w_out)

    return jax.shard_map(local_layer, mesh=mesh, in_specs=(P("data", "seq", None), P("data"), P(None, None), P(), P("seq", None, None), P("seq", None, None)), out_specs=P("data", "seq", None), check_vma=False)
```

```python
import functools

import jax
import jax.numpy as jnp
from jax import lax
from jax.experimental import pallas as pl
from jax.experimental.pallas import tpu as pltpu
from jax.sharding import PartitionSpec as P

EPSILON = 1e-6
NEG_FILL = -1e30
MESH = pl.DeviceIdType.MESH
F32 = jnp.float32
BF16 = jnp.bfloat16
FF_BLOCK = 1024
JOBS = "UAAAU"
ORDER = (("U", 0), ("A", 0), ("A", 1), ("P", 0), ("A", 2), ("P", 1), ("U", 1), ("P", 2))
SCHEDULE = {4: "o0", 8: "o1", 9: "f0", 12: "o2", 13: "f1 o3", 14: "t0", 16: "m0 o4", 17: "t1 f2 o5", 18: "f3", 19: "m1", 20: "o6 t2 f4 t3 o7 f5 m2 f6 m3 t4 f7 t5 m4 t6 m5 t7 m6 m7"}
AHEAD = 12
VMEM_BYTES = 62 * 1024 * 1024


def unit_rows(values):
    v32 = values.astype(F32)
    return (v32 * lax.rsqrt(jnp.sum(v32 * v32, axis=1, keepdims=True) + EPSILON)).astype(BF16)


class Exchange:
    def __init__(self, me, n, chunk, send_sem, recv_sem):
        core = lax.rem(me, 2)
        self.me, self.mate = me, me + 1 - 2 * core
        self.right, self.left = lax.rem(me + 2, n), lax.rem(me + n - 2, n)
        self.far = lax.rem(me + n // 2, n)
        self.rightm, self.leftm, self.farm = (p + 1 - 2 * core for p in (self.right, self.left, self.far))
        self.chunk, self.send_sem, self.recv_sem = chunk, send_sem, recv_sem

    def copy(self, i, half, src, to):
        ref = self.chunk(half, src)
        return pltpu.make_async_remote_copy(src_ref=ref, dst_ref=ref, send_sem=self.send_sem(i), recv_sem=self.recv_sem(half, src), device_id={"seq": to}, device_id_type=MESH)

    def plan(self):
        return [(0, self.me, self.right), (1, self.me, self.right), (1, self.me, self.left), (0, self.me, self.left), (0, self.me, self.mate), (1, self.me, self.mate),
                (0, self.left, self.right), (1, self.right, self.left), (0, self.left, self.mate), (1, self.right, self.mate),
                (1, self.left, self.mate), (0, self.right, self.mate), (0, self.far, self.mate), (1, self.far, self.mate)]

    def start(self, first, last):
        for i, (half, src, to) in list(enumerate(self.plan()))[first:last]:
            self.copy(i, half, src, to).start()

    def arrived(self, *pairs):
        for half, src in pairs:
            self.copy(0, half, src, self.mate).wait_recv()

    def own(self):
        self.start(0, 6)

    def first(self):
        self.arrived((0, self.left), (1, self.right))
        self.start(6, 10)

    def second(self):
        self.arrived((1, self.left), (0, self.right))
        self.start(10, 12)

    def third(self):
        self.arrived((0, self.far), (1, self.far))
        self.start(12, 14)

    def from_mate(self, *sources):
        for src in sources:
            self.arrived((0, src), (1, src))

    def sent(self):
        for i, (half, src, to) in enumerate(self.plan()):
            self.copy(i, half, src, to).wait_send()


def kernel(n, tok_hbm, len_ref, phi_hbm, g_ref, w1_hbm, w2_hbm, out_ref, xall, phi, pnt, lt, cbuf, qbuf, cperm, xs, xpair, ysall, yback, hidden, yexp, yacc, w1buf, w2buf,
           loc_sem, w1_sem, w2_sem, tok_send, tok_recv, ys_send, ys_recv, xp_send, xp_recv, yb_send, yb_recv):
    batch, _, toks, d_model = xall.shape
    n_exp, _, rows, _ = ysall.shape
    per_exp = rows // batch
    slot_loc = n_exp * per_exp
    blocks = w1_hbm.shape[2] // FF_BLOCK
    ahead = w1buf.shape[0]
    chips = n // 2
    me = lax.axis_index("seq")
    g = g_ref[0]

    data = lax.axis_index("data")
    odd = lax.rem(data, 2)
    pair = data + 1 - 2 * odd
    shared = JOBS.count("A")

    def expert_of(kind, k):
        if kind == "U":
            return k if k < JOBS.index("A") else k + 2 * shared
        return JOBS.index("A") + shared * (odd if kind == "A" else 1 - odd) + k

    job_of = [(kind, JOBS[:i].count(kind)) for i, kind in enumerate(JOBS)]
    units = len(JOBS) * blocks

    def w1_copy(u):
        e, f0 = expert_of(*job_of[u // blocks]), u % blocks * FF_BLOCK
        return pltpu.make_async_copy(w1_hbm.at[e, :, pl.ds(f0, FF_BLOCK)], w1buf.at[u % ahead], w1_sem.at[u % ahead])

    def w2_copy(u):
        e, f0 = expert_of(*job_of[u // blocks]), u % blocks * FF_BLOCK
        return pltpu.make_async_copy(w2_hbm.at[e, pl.ds(f0, FF_BLOCK), :], w2buf.at[u % ahead], w2_sem.at[u % ahead])

    def x_to_pair(k):
        return pltpu.make_async_remote_copy(src_ref=xs.at[expert_of("P", k)], dst_ref=xpair.at[k, pl.ds(rows, rows)], send_sem=xp_send.at[k], recv_sem=xp_recv.at[k], device_id={"data": pair}, device_id_type=MESH)

    def y_to_pair(k):
        return pltpu.make_async_remote_copy(src_ref=yback.at[k], dst_ref=ysall.at[ORDER.index(("P", k)), me], send_sem=yb_send.at[k], recv_sem=yb_recv.at[k], device_id={"data": pair}, device_id_type=MESH)

    tok_ex = Exchange(me, n, lambda half, src: xall.at[half, src], lambda i: tok_send.at[i], lambda half, src: tok_recv.at[half, src])
    barrier = pltpu.get_barrier_semaphore()
    for peer in (tok_ex.right, tok_ex.left, tok_ex.mate):
        pl.semaphore_signal(barrier, inc=1, device_id={"seq": peer}, device_id_type=MESH)
    pl.semaphore_signal(barrier, inc=1, device_id={"data": pair}, device_id_type=MESH)
    own_in = [pltpu.make_async_copy(tok_hbm.at[b], xall.at[b, me], loc_sem.at[b]) for b in range(batch)]
    for c in own_in:
        c.start()
    phi_in = pltpu.make_async_copy(phi_hbm, phi, loc_sem.at[batch])
    phi_in.start()

    for c in own_in:
        c.wait()
    pl.semaphore_wait(barrier, 4)
    tok_ex.own()
    for u in range(min(ahead, units)):
        w1_copy(u).start()
        w2_copy(u).start()

    phi_in.wait()
    d_rows = phi.shape[0]
    n_slots = phi.shape[1]
    step = 64

    def sum_sq(i, acc):
        v = phi[pl.ds(pl.multiple_of(i * step, step), step), :].astype(F32)
        return acc + jnp.sum((v * v).reshape(step // 8, 8, n_slots), axis=0)

    scale = lax.rsqrt(jnp.sum(lax.fori_loop(0, d_rows // step, sum_sq, jnp.zeros((8, n_slots), F32)), axis=0, keepdims=True) + EPSILON)

    def to_unit(i, _):
        at = pl.ds(pl.multiple_of(i * step, step), step)
        phi[at, :] = (phi[at, :].astype(F32) * scale).astype(BF16)
        return 0

    lax.fori_loop(0, d_rows // step, to_unit, 0)
    pnt[...] = phi[:, pl.ds(pl.multiple_of(me * slot_loc, slot_loc), slot_loc)].astype(F32).T.astype(BF16)

    for b in range(batch):
        logits = g * jnp.dot(unit_rows(xall[b, me]), phi[...], preferred_element_type=F32)
        comb = jnp.exp(logits - jnp.max(logits, axis=1, keepdims=True))
        at = pl.ds(b * toks, toks)
        qbuf[at, :] = jnp.broadcast_to(jnp.sum(comb, axis=1, keepdims=True), (toks, 128))
        cbuf[at, :] = comb.astype(BF16)

    tok_ex.first()

    def regroup():
        j = lax.broadcasted_iota(jnp.int32, (n_slots, slot_loc), 0)
        k = lax.broadcasted_iota(jnp.int32, (n_slots, slot_loc), 1)
        first = j - ((k // per_exp) * slot_loc + lax.rem(k, per_exp))
        for r, what in enumerate(ORDER):
            pick = (first == expert_of(*what) * per_exp).astype(F32).astype(BF16)
            cperm[r] = jnp.dot(cbuf[...], pick, preferred_element_type=F32).astype(BF16)

    regroup()

    def chip_logits(chip):
        for b in range(batch):
            x_chip = xall[b, pl.ds(2 * chip, 2)].reshape(2 * toks, d_model)
            logits = g * lax.dot_general(pnt[...], unit_rows(x_chip), (((1,), (1,)), ((), ())), preferred_element_type=F32)
            pos = chip * (2 * toks) + lax.broadcasted_iota(jnp.int32, logits.shape, 1)
            lt[b, chip] = jnp.where(pos < len_ref[b], logits, NEG_FILL)

    tok_ex.from_mate(tok_ex.mate)
    chip_logits(me // 2)
    tok_ex.second()
    tok_ex.from_mate(tok_ex.leftm, tok_ex.rightm)
    chip_logits(tok_ex.left // 2)
    chip_logits(tok_ex.right // 2)
    tok_ex.third()
    tok_ex.from_mate(tok_ex.farm)
    chip_logits(tok_ex.far // 2)

    for b in range(batch):
        parts = [lt[b, k] for k in range(chips)]
        top = jnp.max(functools.reduce(jnp.maximum, parts), axis=1, keepdims=True)
        disp = [jnp.exp(p - top) for p in parts]
        col_sum = jnp.sum(functools.reduce(jnp.add, disp), axis=1, keepdims=True)
        weights = jnp.concatenate([w.astype(BF16) for w in disp], axis=1)
        slot_sum = jnp.dot(weights, xall[b].reshape(n * toks, d_model), preferred_element_type=F32)
        xs[:, pl.ds(b * per_exp, per_exp), :] = (slot_sum / col_sum).astype(BF16).reshape(n_exp, per_exp, d_model)
    for k in range(shared):
        x_to_pair(k).start()
        xpair[k, pl.ds(0, rows)] = xs[expert_of("A", k)]
    tok_ex.sent()
    yacc[...] = jnp.zeros_like(yacc)

    def ys_ex(r):
        return Exchange(me, n, lambda half, src: ysall.at[r, src, pl.ds(half * per_exp, per_exp)], lambda i: ys_send.at[r, i], lambda half, src: ys_recv.at[r, half, src])

    def combine(r):
        for b in range(batch):
            at = pl.ds(b * toks, toks)
            got = ysall[r, :, pl.ds(b * per_exp, per_exp), :].reshape(n * per_exp, d_model)
            yacc[at, :] += jnp.dot(cperm[r, at, :], got, preferred_element_type=F32)

    def act(what):
        kind, r = what[0], int(what[1:])
        ex = ys_ex(r)
        with jax.named_scope(what):
            if kind == "o":
                if ORDER[r][0] == "P":
                    y_to_pair(ORDER[r][1]).wait_recv()
                ex.own()
            if kind == "f":
                ex.first()
                ex.second()
            if kind == "t":
                ex.third()
            if kind == "m":
                ex.from_mate(ex.mate, ex.leftm, ex.rightm, ex.farm)
                combine(r)

    for b in range(units + 1):
        with jax.named_scope(f"block{b}"):
            if b < units:
                kind, k = job_of[b // blocks]
                if kind == "A" and b % blocks == 0:
                    x_to_pair(k).wait_recv()
                w1_copy(b).wait()
            if b > 0:
                w2_copy(b - 1).wait()
            if b < units:
                x_job = xs[expert_of(kind, k)] if kind == "U" else xpair[k]
                pre = jnp.dot(x_job, w1buf[b % ahead], preferred_element_type=F32)
            if b > 0:
                done, dk = job_of[(b - 1) // blocks]
                live = pl.ds(0, rows if done == "U" else 2 * rows)
                part = jnp.dot(hidden[(b - 1) % 2, live, :], w2buf[(b - 1) % ahead], preferred_element_type=F32)
                if (b - 1) % blocks:
                    part = yexp[live, :] + part
                if b % blocks:
                    yexp[live, :] = part
                else:
                    ysall[ORDER.index((done, dk)), me] = part[:rows].astype(BF16)
                    if done == "A":
                        yback[dk] = part[rows:].astype(BF16)
            if b < units:
                hidden[b % 2, pl.ds(0, pre.shape[0]), :] = jax.nn.gelu(pre).astype(BF16)
        if b + ahead < units:
            w1_copy(b + ahead).start()
        if 0 < b <= units - ahead:
            w2_copy(b - 1 + ahead).start()
        if b > 0 and b % blocks == 0 and done == "A":
            y_to_pair(dk).start()
        for what in SCHEDULE.get(b, "").split():
            act(what)
    for r in range(n_exp):
        ys_ex(r).sent()
    for k in range(shared):
        x_to_pair(k).wait_send()
        y_to_pair(k).wait_send()

    for b in range(batch):
        at = pl.ds(b * toks, toks)
        pos = me * toks + lax.broadcasted_iota(jnp.int32, (toks, 1), 0)
        out_ref[b] = jnp.where(pos < len_ref[b], yacc[at, :] / qbuf[at, 0:1], 0.0).astype(BF16)


def solution(mesh):
    n = mesh.shape["seq"]

    def local_layer(tok_blk, len_blk, slot_param, logit_scale, w_in, w_out):
        batch, toks, d_model = tok_blk.shape
        n_slots = slot_param.shape[1]
        n_exp = w_in.shape[0]
        slot_loc = n_slots // n
        rows = batch * (slot_loc // n_exp)
        dma = pltpu.SemaphoreType.DMA
        any_spec = pl.BlockSpec(memory_space=pl.ANY)
        smem_spec = pl.BlockSpec(memory_space=pltpu.SMEM)
        return pl.pallas_call(
            functools.partial(kernel, n),
            out_shape=pltpu.VMEM(tok_blk.shape, BF16),
            in_specs=[any_spec, smem_spec, any_spec, smem_spec, any_spec, any_spec],
            out_specs=pl.BlockSpec(memory_space=pltpu.VMEM),
            scratch_shapes=[
                pltpu.VMEM((batch, n, toks, d_model), BF16),
                pltpu.VMEM(slot_param.shape, BF16),
                pltpu.VMEM((slot_loc, d_model), BF16),
                pltpu.VMEM((batch, n // 2, slot_loc, 2 * toks), F32),
                pltpu.VMEM((batch * toks, n_slots), BF16),
                pltpu.VMEM((batch * toks, 128), F32),
                pltpu.VMEM((n_exp, batch * toks, n_slots // n_exp), BF16),
                pltpu.VMEM((n_exp, rows, d_model), BF16),
                pltpu.VMEM((JOBS.count("A"), 2 * rows, d_model), BF16),
                pltpu.VMEM((n_exp, n, rows, d_model), BF16),
                pltpu.VMEM((JOBS.count("A"), rows, d_model), BF16),
                pltpu.VMEM((2, 2 * rows, FF_BLOCK), BF16),
                pltpu.VMEM((2 * rows, d_model), F32),
                pltpu.VMEM((batch * toks, d_model), F32),
                pltpu.VMEM((AHEAD, d_model, FF_BLOCK), BF16),
                pltpu.VMEM((AHEAD, FF_BLOCK, d_model), BF16),
                dma((batch + 1,)), dma((AHEAD,)), dma((AHEAD,)),
                dma((14,)), dma((batch, n)), dma((n_exp, 14)), dma((n_exp, batch, n)),
                *[dma((JOBS.count("A"),))] * 4,
            ],
            compiler_params=pltpu.CompilerParams(collective_id=0, has_side_effects=True, vmem_limit_bytes=VMEM_BYTES),
        )(tok_blk, len_blk, slot_param, logit_scale.reshape(1), w_in, w_out)

    return jax.shard_map(local_layer, mesh=mesh, in_specs=(P("data", "seq", None), P("data"), P(None, None), P(), P("seq", None, None), P("seq", None, None)), out_specs=P("data", "seq", None), check_vma=False)
```

```python
import functools

import jax
import jax.numpy as jnp
from jax import lax
from jax.experimental import pallas as pl
from jax.experimental.pallas import tpu as pltpu
from jax.sharding import PartitionSpec as P

EPSILON = 1e-6
NEG_FILL = -1e30
MESH = pl.DeviceIdType.MESH
F32 = jnp.float32
BF16 = jnp.bfloat16
FF_BLOCK = 1024
JOBS = (("U", 0, 0), ("U", 1, None), ("A", 0, None), ("A", 1, None), ("A", 2, None), ("U", 0, 1))
EXPERTS = (("U", 0), ("A", 0), ("A", 1), ("P", 0), ("A", 2), ("P", 1), ("U", 1), ("P", 2))
RINGS = (("U", 0, 0), ("U", 1, None), ("A", 0, None), ("A", 1, None), ("P", 0, None), ("A", 2, None), ("P", 1, None), ("U", 0, 1), ("P", 2, None))
BEFORE, SHARED = 1, 3
PROGRAM = (
    "B2", "S1", "B1", "T1", "B1", "L1", "D1", "B1", "o0", "B1", "B1", "B1", "B1", "f0", "s0", "o1", "B1", "B1", "B1", "B1", "t0", "o2",
    "B1", "f1", "B1", "m0", "s1", "B1", "B1", "o3", "f2", "B1", "o4", "s2", "B1", "t1", "B1", "B1", "o5", "m1", "f3", "B1", "o6", "s3",
    "B2", "t2", "B1", "f4", "o7", "s4", "t3", "o8", "f5", "s5", "m2", "f6", "s6", "t4", "f7", "s7", "m3", "f8", "s8", "t5", "t6", "m4",
    "t7", "t8", "m5", "m6", "m7", "m8",
)
AHEAD = 12
VMEM_BYTES = 62 * 1024 * 1024


def unit_rows(values):
    v32 = values.astype(F32)
    return (v32 * lax.rsqrt(jnp.sum(v32 * v32, axis=1, keepdims=True) + EPSILON)).astype(BF16)


FIRST, SECOND, THIRD, MATE, MATE_NEAR, MATE_FAR = range(6)


class Exchange:
    def __init__(self, me, n, chunk, span, send_sem, recv_sem, groups):
        core = lax.rem(me, 2)
        self.me, self.mate = me, me + 1 - 2 * core
        self.right, self.left = lax.rem(me + 2, n), lax.rem(me + n - 2, n)
        self.far = lax.rem(me + n // 2, n)
        self.chunk, self.span, self.send_sem, self.recv_sem, self.groups = chunk, span, send_sem, recv_sem, groups

    def plan(self):
        me, right, left, far, mate = self.me, self.right, self.left, self.far, self.mate
        return [(0, me, right, FIRST), (1, me, right, SECOND), (1, me, left, FIRST), (0, me, left, SECOND), (0, me, mate, MATE), (1, me, mate, MATE),
                (0, left, right, THIRD), (1, right, left, THIRD), (0, left, mate, MATE_NEAR), (1, right, mate, MATE_NEAR),
                (1, left, mate, MATE_NEAR), (0, right, mate, MATE_NEAR), (0, far, mate, MATE_FAR), (1, far, mate, MATE_FAR)]

    def start(self, *which):
        for half, src, to, group in (self.plan()[i] for i in which):
            ref = self.chunk(half, src)
            pltpu.make_async_remote_copy(src_ref=ref, dst_ref=ref, send_sem=self.send_sem, recv_sem=self.recv_sem(self.groups[group]), device_id={"seq": to}, device_id_type=MESH).start()

    def arrived(self, group, pairs):
        ref = self.span(pairs)
        pltpu.make_async_remote_copy(src_ref=ref, dst_ref=ref, send_sem=self.send_sem, recv_sem=self.recv_sem(group), device_id={"seq": self.mate}, device_id_type=MESH).wait_recv()

    def own(self):
        self.start(0, 1, 2, 3, 4, 5)

    def first(self):
        self.arrived(FIRST, 1)
        self.start(6, 7, 8, 9)

    def second(self):
        self.arrived(SECOND, 1)
        self.start(10, 11)

    def third(self):
        self.arrived(THIRD, 1)
        self.start(12, 13)

    def sent(self):
        ref = self.span(7)
        pltpu.make_async_remote_copy(src_ref=ref, dst_ref=ref, send_sem=self.send_sem, recv_sem=self.recv_sem(0), device_id={"seq": self.mate}, device_id_type=MESH).wait_send()


def kernel(n, tok_hbm, len_hbm, phi_hbm, g_ref, w1_hbm, w2_hbm, out_ref, xall, phi, pnt, lt, cbuf, qbuf, cperm, xs, xpair, ysall, yback, hidden, yexp, yacc, w1buf, w2buf,
           loc_sem, w1_sem, w2_sem, tok_send, tok_recv, ys_send, ys_recv, xp_send, xp_recv, yb_send, yb_recv, len_ref):
    batch, _, toks, d_model = xall.shape
    n_exp, _, rows, _ = ysall.shape
    per_exp = rows // batch
    slot_loc = n_exp * per_exp
    blocks = w1_hbm.shape[2] // FF_BLOCK
    ahead = w1buf.shape[0]
    chips = n // 2
    me = lax.axis_index("seq")
    g = g_ref[0]

    data = lax.axis_index("data")
    odd = lax.rem(data, 2)
    pair = data + 1 - 2 * odd

    def expert_of(kind, k):
        if kind == "U":
            return k if k < BEFORE else k + 2 * SHARED
        return BEFORE + SHARED * (odd if kind == "A" else 1 - odd) + k

    loads = list(dict.fromkeys((kind, k) for kind, k, _ in JOBS))
    n_loads = len(loads) * blocks
    units = len(JOBS) * blocks

    def job_of(b):
        return JOBS[b // blocks]

    def load_of(b):
        return loads.index(job_of(b)[:2]) * blocks + b % blocks

    def used_again(b):
        return any(load_of(later) == load_of(b) for later in range(b + 1, units))

    def used_before(b):
        return any(load_of(early) == load_of(b) for early in range(b))

    def slot_of(u):
        return u if u < ahead else blocks + (u - ahead) % (ahead - blocks)

    def next_load(u):
        return next((v for v in range(u + 1, n_loads) if slot_of(v) == slot_of(u)), None)

    def w1_copy(u):
        e, f0 = expert_of(*loads[u // blocks]), u % blocks * FF_BLOCK
        return pltpu.make_async_copy(w1_hbm.at[e, :, pl.ds(f0, FF_BLOCK)], w1buf.at[slot_of(u)], w1_sem.at[slot_of(u)])

    def w2_copy(u):
        e, f0 = expert_of(*loads[u // blocks]), u % blocks * FF_BLOCK
        return pltpu.make_async_copy(w2_hbm.at[e, pl.ds(f0, FF_BLOCK), :], w2buf.at[slot_of(u)], w2_sem.at[slot_of(u)])

    def x_to_pair(k, b):
        src, dst = pl.ds(b * per_exp, per_exp), pl.ds(rows + b * per_exp, per_exp)
        return pltpu.make_async_remote_copy(src_ref=xs.at[expert_of("P", k), src], dst_ref=xpair.at[k, dst], send_sem=xp_send.at[0], recv_sem=xp_recv.at[k], device_id={"data": pair}, device_id_type=MESH)

    def y_to_pair(k):
        return pltpu.make_async_remote_copy(src_ref=yback.at[k], dst_ref=ysall.at[EXPERTS.index(("P", k)), me], send_sem=yb_send.at[0], recv_sem=yb_recv.at[k], device_id={"data": pair}, device_id_type=MESH)

    part = toks // 2
    tok0, tok1 = (Exchange(me, n, lambda half, src, b=b: xall.at[b, src, pl.ds(half * part, part)], lambda pairs, b=b: xall.at[b, pl.ds(0, pairs)], tok_send.at[b], lambda group, b=b: tok_recv.at[b, group], range(6)) for b in range(batch))
    barrier = pltpu.get_barrier_semaphore()
    for peer in (tok0.right, tok0.left, tok0.mate):
        pl.semaphore_signal(barrier, inc=1, device_id={"seq": peer}, device_id_type=MESH)
    pl.semaphore_signal(barrier, inc=1, device_id={"data": pair}, device_id_type=MESH)
    own_in = [pltpu.make_async_copy(tok_hbm.at[b], xall.at[b, me], loc_sem.at[b]) for b in range(batch)]
    for c in own_in:
        c.start()
    phi_in = pltpu.make_async_copy(phi_hbm, phi, loc_sem.at[batch])
    phi_in.start()
    len_in = pltpu.make_async_copy(len_hbm, len_ref, loc_sem.at[batch + 1])
    len_in.start()

    for c in own_in:
        c.wait()
    for u in range(min(ahead, n_loads)):
        w1_copy(u).start()
        w2_copy(u).start()
    pl.semaphore_wait(barrier, 4)
    tok0.own()
    tok1.start(0, 2)

    phi_in.wait()
    len_in.wait()
    d_rows = phi.shape[0]
    n_slots = phi.shape[1]
    step = 64

    def sum_sq(i, acc):
        v = phi[pl.ds(pl.multiple_of(i * step, step), step), :].astype(F32)
        return acc + jnp.sum((v * v).reshape(step // 8, 8, n_slots), axis=0)

    scale = lax.rsqrt(jnp.sum(lax.fori_loop(0, d_rows // step, sum_sq, jnp.zeros((8, n_slots), F32)), axis=0, keepdims=True) + EPSILON)

    def to_unit(i, _):
        at = pl.ds(pl.multiple_of(i * step, step), step)
        phi[at, :] = (phi[at, :].astype(F32) * scale).astype(BF16)
        return 0

    lax.fori_loop(0, d_rows // step, to_unit, 0)
    pnt[...] = phi[:, pl.ds(pl.multiple_of(me * slot_loc, slot_loc), slot_loc)].astype(F32).T.astype(BF16)

    for b in range(batch):
        logits = g * jnp.dot(unit_rows(xall[b, me]), phi[...], preferred_element_type=F32)
        comb = jnp.exp(logits - jnp.max(logits, axis=1, keepdims=True))
        at = pl.ds(b * toks, toks)
        qbuf[at, :] = jnp.broadcast_to(jnp.sum(comb, axis=1, keepdims=True), (toks, 128))
        cbuf[at, :] = comb.astype(BF16)

    tok0.first()
    tok1.start(1, 3, 4, 5)

    def regroup():
        j = lax.broadcasted_iota(jnp.int32, (n_slots, slot_loc), 0)
        k = lax.broadcasted_iota(jnp.int32, (n_slots, slot_loc), 1)
        first = j - ((k // per_exp) * slot_loc + lax.rem(k, per_exp))
        for r, what in enumerate(EXPERTS):
            pick = (first == expert_of(*what) * per_exp).astype(F32).astype(BF16)
            cperm[r] = jnp.dot(cbuf[...], pick, preferred_element_type=F32).astype(BF16)

    regroup()

    def chip_logits(b, src):
        chip = src // 2
        x_chip = xall[b, pl.ds(2 * chip, 2)].reshape(2 * toks, d_model)
        logits = g * lax.dot_general(pnt[...], unit_rows(x_chip), (((1,), (1,)), ((), ())), preferred_element_type=F32)
        pos = chip * (2 * toks) + lax.broadcasted_iota(jnp.int32, logits.shape, 1)
        lt[b, chip] = jnp.where(pos < len_ref[b], logits, NEG_FILL)

    def dispatch(b):
        parts = [lt[b, k] for k in range(chips)]
        top = jnp.max(functools.reduce(jnp.maximum, parts), axis=1, keepdims=True)
        disp = [jnp.exp(p - top) for p in parts]
        col_sum = jnp.sum(functools.reduce(jnp.add, disp), axis=1, keepdims=True)
        weights = jnp.concatenate([w.astype(BF16) for w in disp], axis=1)
        slot_sum = jnp.dot(weights, xall[b].reshape(n * toks, d_model), preferred_element_type=F32)
        at = pl.ds(b * per_exp, per_exp)
        xs[:, at, :] = (slot_sum / col_sum).astype(BF16).reshape(n_exp, per_exp, d_model)
        for k in range(SHARED):
            x_to_pair(k, b).start()
            xpair[k, at] = xs[expert_of("A", k), at]

    tok0.second()
    tok0.arrived(MATE, 1)
    chip_logits(0, me)
    tok1.first()
    tok0.third()
    tok0.arrived(MATE_NEAR, 2)
    chip_logits(0, tok0.left)
    chip_logits(0, tok0.right)
    tok0.arrived(MATE_FAR, 1)
    chip_logits(0, tok0.far)
    dispatch(0)
    yacc[...] = jnp.zeros_like(yacc)

    def ys_ex(r):
        kind, k, only = RINGS[r]
        buf, half_d = EXPERTS.index((kind, k)), d_model // 2

        def chunk(half, src):
            if only is None:
                return ysall.at[buf, src, pl.ds(half * per_exp, per_exp)]
            return ysall.at[buf, src, pl.ds(only * per_exp, per_exp), pl.ds(half * half_d, half_d)]

        def span(pairs):
            if only is None:
                return ysall.at[buf, pl.ds(0, pairs)]
            return ysall.at[buf, pl.ds(0, pairs), pl.ds(only * per_exp, per_exp)]

        return Exchange(me, n, chunk, span, ys_send.at[r], lambda group: ys_recv.at[r, group], (FIRST, SECOND, THIRD, MATE, MATE, MATE))

    def combine(r):
        kind, k, only = RINGS[r]
        buf = EXPERTS.index((kind, k))
        for b in range(batch) if only is None else (only,):
            at = pl.ds(b * toks, toks)
            got = ysall[buf, :, pl.ds(b * per_exp, per_exp), :].reshape(n * per_exp, d_model)
            yacc[at, :] += jnp.dot(cperm[buf, at, :], got, preferred_element_type=F32)

    def run_blocks(todo):
        for b in todo:
            if b < units:
                kind, k, only = job_of(b)
                if kind == "A" and b % blocks == 0:
                    whole = xpair.at[k, pl.ds(rows, rows)]
                    pltpu.make_async_remote_copy(src_ref=whole, dst_ref=whole, send_sem=xp_send.at[0], recv_sem=xp_recv.at[k], device_id={"data": pair}, device_id_type=MESH).wait_recv()
                if not used_before(b):
                    w1_copy(load_of(b)).wait()
            if b > 0 and not used_before(b - 1):
                w2_copy(load_of(b - 1)).wait()
        back = []
        for b in todo:
            if b < units:
                kind, k, only = job_of(b)
                if kind == "A":
                    x_job = xpair[k]
                elif only is None:
                    x_job = xs[expert_of(kind, k)]
                else:
                    x_job = xs[expert_of(kind, k), pl.ds(only * per_exp, per_exp)]
                pre = jnp.dot(x_job, w1buf[slot_of(load_of(b))], preferred_element_type=F32)
            if b > 0:
                kind, k, only = job_of(b - 1)
                live = pl.ds(0, 2 * rows if kind == "A" else rows if only is None else per_exp)
                out = jnp.dot(hidden[(b - 1) % 2, live, :], w2buf[slot_of(load_of(b - 1))], preferred_element_type=F32)
                if (b - 1) % blocks:
                    out = yexp[live, :] + out
                if b % blocks:
                    yexp[live, :] = out
                else:
                    buf = EXPERTS.index((kind, k))
                    if only is None:
                        ysall[buf, me] = out[:rows].astype(BF16)
                    else:
                        ysall[buf, me, pl.ds(only * per_exp, per_exp)] = out.astype(BF16)
                    if kind == "A":
                        yback[k] = out[rows:].astype(BF16)
                        back.append(k)
            if b < units:
                hidden[b % 2, pl.ds(0, pre.shape[0]), :] = jax.nn.gelu(pre).astype(BF16)
        for b in todo:
            if b < units and not used_again(b) and next_load(load_of(b)) is not None:
                w1_copy(next_load(load_of(b))).start()
            if b > 0 and not used_again(b - 1) and next_load(load_of(b - 1)) is not None:
                w2_copy(next_load(load_of(b - 1))).start()
        for k in back:
            y_to_pair(k).start()

    def act(kind, r):
        if kind == "S":
            tok1.second()
        elif kind == "L":
            tok1.arrived(MATE, 1)
            tok1.arrived(MATE_NEAR, 2)
            for src in (me, tok1.left, tok1.right):
                chip_logits(1, src)
        elif kind == "T":
            tok1.third()
        elif kind == "D":
            tok1.arrived(MATE_FAR, 1)
            chip_logits(1, tok1.far)
            dispatch(1)
        elif kind == "o":
            if RINGS[r][0] == "P":
                y_to_pair(RINGS[r][1]).wait_recv()
            ys_ex(r).own()
        elif kind == "f":
            ys_ex(r).first()
        elif kind == "s":
            ys_ex(r).second()
        elif kind == "t":
            ys_ex(r).third()
        else:
            ys_ex(r).arrived(MATE, 4)
            combine(r)

    done = 0
    for what in PROGRAM:
        kind, r = what[0], int(what[1:])
        with jax.named_scope(what if kind != "B" else f"B{done}"):
            if kind == "B":
                run_blocks(range(done, done + r))
                done += r
            else:
                act(kind, r)
    with jax.named_scope("final"):
        for b in range(batch):
            at = pl.ds(b * toks, toks)
            pos = me * toks + lax.broadcasted_iota(jnp.int32, (toks, 1), 0)
            out_ref[b] = jnp.where(pos < len_ref[b], yacc[at, :] / qbuf[at, 0:1], 0.0).astype(BF16)
    with jax.named_scope("sent"):
        for ex in (tok0, tok1, *(ys_ex(r) for r in range(len(RINGS)))):
            ex.sent()
        pltpu.make_async_remote_copy(src_ref=yback, dst_ref=yback, send_sem=xp_send.at[0], recv_sem=xp_recv.at[0], device_id={"data": pair}, device_id_type=MESH).wait_send()
        pltpu.make_async_remote_copy(src_ref=yback, dst_ref=yback, send_sem=yb_send.at[0], recv_sem=yb_recv.at[0], device_id={"data": pair}, device_id_type=MESH).wait_send()


def solution(mesh):
    n = mesh.shape["seq"]

    def local_layer(tok_blk, len_blk, slot_param, logit_scale, w_in, w_out):
        batch, toks, d_model = tok_blk.shape
        n_slots = slot_param.shape[1]
        n_exp = w_in.shape[0]
        slot_loc = n_slots // n
        rows = batch * (slot_loc // n_exp)
        dma = pltpu.SemaphoreType.DMA
        any_spec = pl.BlockSpec(memory_space=pl.ANY)
        smem_spec = pl.BlockSpec(memory_space=pltpu.SMEM)
        return pl.pallas_call(
            functools.partial(kernel, n),
            out_shape=pltpu.VMEM(tok_blk.shape, BF16),
            in_specs=[any_spec, any_spec, any_spec, smem_spec, any_spec, any_spec],
            out_specs=pl.BlockSpec(memory_space=pltpu.VMEM),
            scratch_shapes=[
                pltpu.VMEM((batch, n, toks, d_model), BF16),
                pltpu.VMEM(slot_param.shape, BF16),
                pltpu.VMEM((slot_loc, d_model), BF16),
                pltpu.VMEM((batch, n // 2, slot_loc, 2 * toks), F32),
                pltpu.VMEM((batch * toks, n_slots), BF16),
                pltpu.VMEM((batch * toks, 128), F32),
                pltpu.VMEM((n_exp, batch * toks, n_slots // n_exp), BF16),
                pltpu.VMEM((n_exp, rows, d_model), BF16),
                pltpu.VMEM((SHARED, 2 * rows, d_model), BF16),
                pltpu.VMEM((n_exp, n, rows, d_model), BF16),
                pltpu.VMEM((SHARED, rows, d_model), BF16),
                pltpu.VMEM((2, 2 * rows, FF_BLOCK), BF16),
                pltpu.VMEM((2 * rows, d_model), F32),
                pltpu.VMEM((batch * toks, d_model), F32),
                pltpu.VMEM((AHEAD, d_model, FF_BLOCK), BF16),
                pltpu.VMEM((AHEAD, FF_BLOCK, d_model), BF16),
                dma((batch + 2,)), dma((AHEAD,)), dma((AHEAD,)),
                dma((batch,)), dma((batch, 6)), dma((len(RINGS),)), dma((len(RINGS), 4)),
                dma((1,)), dma((SHARED,)), dma((1,)), dma((SHARED,)),
                pltpu.SMEM((batch,), jnp.int32),
            ],
            compiler_params=pltpu.CompilerParams(collective_id=0, has_side_effects=True, vmem_limit_bytes=VMEM_BYTES),
        )(tok_blk, len_blk, slot_param, logit_scale.reshape(1), w_in, w_out)

    return jax.shard_map(local_layer, mesh=mesh, in_specs=(P("data", "seq", None), P("data"), P(None, None), P(), P("seq", None, None), P("seq", None, None)), out_specs=P("data", "seq", None), check_vma=False)
```

```python
import functools

import jax
import jax.numpy as jnp
from jax import lax
from jax.experimental import pallas as pl
from jax.experimental.pallas import tpu as pltpu
from jax.sharding import PartitionSpec as P

EPSILON = 1e-6
NEG_FILL = -1e30
MESH = pl.DeviceIdType.MESH
F32 = jnp.float32
BF16 = jnp.bfloat16
FF_BLOCK = 1024
JOBS = (("U", 0, 0), ("U", 1, None), ("A", 0, None), ("A", 1, None), ("A", 2, None), ("U", 0, 1))
EXPERTS = (("U", 0), ("A", 0), ("A", 1), ("P", 0), ("A", 2), ("P", 1), ("U", 1), ("P", 2))
RINGS = (("U", 0, 0), ("U", 1, None), ("A", 0, None), ("A", 1, None), ("P", 0, None), ("A", 2, None), ("P", 1, None), ("U", 0, 1), ("P", 2, None))
BEFORE, SHARED = 1, 3
DIRECT = (7,)
PROGRAM = (
    "S1", "B2", "L1", "T1", "B1", "D1", "B1", "B1", "o0", "B1", "B1", "B1", "F1", "o1", "B1", "B1", "f0", "s0", "B1", "B1", "F1", "o2",
    "B1", "f1", "B1", "s1", "B1", "t0", "B1", "B1", "o3", "m0", "B1", "f2", "f4", "B1", "B1", "s2", "s4", "B1", "t1", "o5", "B1", "B1",
    "B1", "f3", "f6", "m1", "F1", "o7", "s3", "s6", "t2", "o4", "t4", "o6", "f5", "f8", "s5", "s8", "t3", "o8", "m2", "t6", "f7", "s7",
    "m4", "t5", "t7", "t8", "m3", "m6", "m5", "m7", "m8",
)
AHEAD = 12
VMEM_BYTES = 62 * 1024 * 1024


def unit_rows(values):
    v32 = values.astype(F32)
    return (v32 * lax.rsqrt(jnp.sum(v32 * v32, axis=1, keepdims=True) + EPSILON)).astype(BF16)


FIRST, SECOND, THIRD, MATE, MATE_NEAR, MATE_FAR = range(6)


class Exchange:
    def __init__(self, me, n, chunk, span, send_sem, recv_sem, groups, direct=False):
        core = lax.rem(me, 2)
        self.me, self.mate = me, me + 1 - 2 * core
        self.right, self.left = lax.rem(me + 2, n), lax.rem(me + n - 2, n)
        self.far = lax.rem(me + n // 2, n)
        self.chunk, self.span, self.send_sem, self.recv_sem, self.groups, self.direct = chunk, span, send_sem, recv_sem, groups, direct

    def plan(self):
        me, right, left, far, mate = self.me, self.right, self.left, self.far, self.mate
        onward = [(0, me, far, THIRD), (1, me, far, THIRD)] if self.direct else [(0, left, right, THIRD), (1, right, left, THIRD)]
        return [(0, me, right, FIRST), (1, me, right, SECOND), (1, me, left, FIRST), (0, me, left, SECOND), (0, me, mate, MATE), (1, me, mate, MATE),
                *onward, (0, left, mate, MATE_NEAR), (1, right, mate, MATE_NEAR),
                (1, left, mate, MATE_NEAR), (0, right, mate, MATE_NEAR), (0, far, mate, MATE_FAR), (1, far, mate, MATE_FAR)]

    def start(self, *which):
        for half, src, to, group in (self.plan()[i] for i in which):
            ref = self.chunk(half, src)
            pltpu.make_async_remote_copy(src_ref=ref, dst_ref=ref, send_sem=self.send_sem, recv_sem=self.recv_sem(self.groups[group]), device_id={"seq": to}, device_id_type=MESH).start()

    def arrived(self, group, pairs):
        ref = self.span(pairs)
        pltpu.make_async_remote_copy(src_ref=ref, dst_ref=ref, send_sem=self.send_sem, recv_sem=self.recv_sem(group), device_id={"seq": self.mate}, device_id_type=MESH).wait_recv()

    def own(self):
        self.start(0, 1, 2, 3, 4, 5, *((6, 7) if self.direct else ()))

    def first(self):
        self.arrived(FIRST, 1)
        self.start(*(() if self.direct else (6, 7)), 8, 9)

    def second(self):
        self.arrived(SECOND, 1)
        self.start(10, 11)

    def third(self):
        self.arrived(THIRD, 1)
        self.start(12, 13)

    def sent(self, pairs=7):
        ref = self.span(pairs)
        pltpu.make_async_remote_copy(src_ref=ref, dst_ref=ref, send_sem=self.send_sem, recv_sem=self.recv_sem(0), device_id={"seq": self.mate}, device_id_type=MESH).wait_send()


def kernel(n, tok_hbm, len_hbm, phi_hbm, g_ref, w1_hbm, w2_hbm, out_ref, xall, phi, pnt, lt, cbuf, qbuf, cperm, xs, xpair, ysall, yback, hidden, yexp, yacc, w1buf, w2buf,
           loc_sem, w1_sem, w2_sem, tok_send, tok_recv, ys_send, ys_recv, xp_send, xp_recv, yb_send, yb_recv, len_ref, pairs_in):
    batch, _, toks, d_model = xall.shape
    n_exp, _, rows, _ = ysall.shape
    per_exp = rows // batch
    slot_loc = n_exp * per_exp
    blocks = w1_hbm.shape[2] // FF_BLOCK
    ahead = w1buf.shape[0]
    chips = n // 2
    me = lax.axis_index("seq")
    g = g_ref[0]

    data = lax.axis_index("data")
    odd = lax.rem(data, 2)
    pair = data + 1 - 2 * odd

    def expert_of(kind, k):
        if kind == "U":
            return k if k < BEFORE else k + 2 * SHARED
        return BEFORE + SHARED * (odd if kind == "A" else 1 - odd) + k

    units = len(JOBS) * blocks

    def job_of(b):
        return JOBS[b // blocks]

    def w1_copy(b):
        e, f0 = expert_of(*job_of(b)[:2]), b % blocks * FF_BLOCK
        return pltpu.make_async_copy(w1_hbm.at[e, :, pl.ds(f0, FF_BLOCK)], w1buf.at[b % ahead], w1_sem.at[b % ahead])

    def w2_copy(b):
        e, f0 = expert_of(*job_of(b)[:2]), b % blocks * FF_BLOCK
        return pltpu.make_async_copy(w2_hbm.at[e, pl.ds(f0, FF_BLOCK), :], w2buf.at[b % ahead], w2_sem.at[b % ahead])

    def x_to_pair(k, b):
        src, dst = pl.ds(b * per_exp, per_exp), pl.ds(rows + b * per_exp, per_exp)
        return pltpu.make_async_remote_copy(src_ref=xs.at[expert_of("P", k), src], dst_ref=xpair.at[k, dst], send_sem=xp_send.at[0], recv_sem=xp_recv.at[k], device_id={"data": pair}, device_id_type=MESH)

    def y_to_pair(k, *which):
        buf = EXPERTS.index(("P", k))
        r = RINGS.index(("P", k, None))
        plan = ((0, tok0.right, ys_recv.at[r, FIRST]), (1, tok0.left, ys_recv.at[r, FIRST]), (1, tok0.right, ys_recv.at[r, SECOND]), (0, tok0.left, ys_recv.at[r, SECOND]), (0, me, yb_recv.at[k]), (1, me, yb_recv.at[k]))
        for half, to, sem in (plan[i] for i in which):
            at = pl.ds(half * per_exp, per_exp)
            pltpu.make_async_remote_copy(src_ref=yback.at[k, at], dst_ref=ysall.at[buf, me, at], send_sem=yb_send.at[0], recv_sem=sem, device_id={"data": pair, "seq": to}, device_id_type=MESH).start()

    part = toks // 2
    tok0, tok1 = (Exchange(me, n, lambda half, src, b=b: xall.at[b, src, pl.ds(half * part, part)], lambda pairs, b=b: xall.at[b, pl.ds(0, pairs)], tok_send.at[b], lambda group, b=b: tok_recv.at[b, group], range(6)) for b in range(batch))
    barrier = pltpu.get_barrier_semaphore()
    for peer in (tok0.right, tok0.left, tok0.mate):
        pl.semaphore_signal(barrier, inc=1, device_id={"seq": peer}, device_id_type=MESH)
    pl.semaphore_signal(barrier, inc=1, device_id={"data": pair}, device_id_type=MESH)
    own_in = [pltpu.make_async_copy(tok_hbm.at[b], xall.at[b, me], loc_sem.at[b]) for b in range(batch)]
    for c in own_in:
        c.start()
    phi_in = pltpu.make_async_copy(phi_hbm, phi, loc_sem.at[batch])
    phi_in.start()
    len_in = pltpu.make_async_copy(len_hbm, len_ref, loc_sem.at[batch + 1])
    len_in.start()

    for c in own_in:
        c.wait()
    for u in range(min(ahead, units)):
        w1_copy(u).start()
        w2_copy(u).start()
    pl.semaphore_wait(barrier, 4)
    tok0.own()
    tok1.start(0, 2)
    for peer in (tok0.right, tok0.left):
        pl.semaphore_signal(pairs_in, inc=1, device_id={"seq": peer}, device_id_type=MESH)

    phi_in.wait()
    len_in.wait()
    d_rows = phi.shape[0]
    n_slots = phi.shape[1]
    step = 64

    def sum_sq(i, acc):
        v = phi[pl.ds(pl.multiple_of(i * step, step), step), :].astype(F32)
        return acc + jnp.sum((v * v).reshape(step // 8, 8, n_slots), axis=0)

    scale = lax.rsqrt(jnp.sum(lax.fori_loop(0, d_rows // step, sum_sq, jnp.zeros((8, n_slots), F32)), axis=0, keepdims=True) + EPSILON)

    def to_unit(i, _):
        at = pl.ds(pl.multiple_of(i * step, step), step)
        phi[at, :] = (phi[at, :].astype(F32) * scale).astype(BF16)
        return 0

    lax.fori_loop(0, d_rows // step, to_unit, 0)
    pnt[...] = phi[:, pl.ds(pl.multiple_of(me * slot_loc, slot_loc), slot_loc)].astype(F32).T.astype(BF16)

    for b in range(batch):
        logits = g * jnp.dot(unit_rows(xall[b, me]), phi[...], preferred_element_type=F32)
        comb = jnp.exp(logits - jnp.max(logits, axis=1, keepdims=True))
        at = pl.ds(b * toks, toks)
        qbuf[at, :] = jnp.broadcast_to(jnp.sum(comb, axis=1, keepdims=True), (toks, 128))
        cbuf[at, :] = comb.astype(BF16)

    tok0.first()
    tok1.start(1, 3, 4, 5)

    def regroup():
        j = lax.broadcasted_iota(jnp.int32, (n_slots, slot_loc), 0)
        k = lax.broadcasted_iota(jnp.int32, (n_slots, slot_loc), 1)
        first = j - ((k // per_exp) * slot_loc + lax.rem(k, per_exp))
        for r, what in enumerate(EXPERTS):
            pick = (first == expert_of(*what) * per_exp).astype(F32).astype(BF16)
            cperm[r] = jnp.dot(cbuf[...], pick, preferred_element_type=F32).astype(BF16)

    regroup()

    def chip_logits(b, src):
        chip = src // 2
        x_chip = xall[b, pl.ds(2 * chip, 2)].reshape(2 * toks, d_model)
        logits = g * lax.dot_general(pnt[...], unit_rows(x_chip), (((1,), (1,)), ((), ())), preferred_element_type=F32)
        pos = chip * (2 * toks) + lax.broadcasted_iota(jnp.int32, logits.shape, 1)
        lt[b, chip] = jnp.where(pos < len_ref[b], logits, NEG_FILL)

    def dispatch(b):
        parts = [lt[b, k] for k in range(chips)]
        top = jnp.max(functools.reduce(jnp.maximum, parts), axis=1, keepdims=True)
        disp = [jnp.exp(p - top) for p in parts]
        col_sum = jnp.sum(functools.reduce(jnp.add, disp), axis=1, keepdims=True)
        weights = jnp.concatenate([w.astype(BF16) for w in disp], axis=1)
        slot_sum = jnp.dot(weights, xall[b].reshape(n * toks, d_model), preferred_element_type=F32)
        at = pl.ds(b * per_exp, per_exp)
        xs[:, at, :] = (slot_sum / col_sum).astype(BF16).reshape(n_exp, per_exp, d_model)
        for k in range(SHARED):
            x_to_pair(k, b).start()
            xpair[k, at] = xs[expert_of("A", k), at]

    tok0.second()
    tok0.arrived(MATE, 1)
    chip_logits(0, me)
    tok1.first()
    tok0.third()
    tok0.arrived(MATE_NEAR, 2)
    chip_logits(0, tok0.left)
    chip_logits(0, tok0.right)
    upper = lax.rem(me, 2) == 1

    @pl.when(upper)
    def _():
        tok1.second()
        tok1.third()

    tok0.arrived(MATE_FAR, 1)
    chip_logits(0, tok0.far)
    dispatch(0)
    pl.semaphore_wait(pairs_in, 2)
    yacc[...] = jnp.zeros_like(yacc)

    def ys_ex(r):
        kind, k, only = RINGS[r]
        buf, half_d = EXPERTS.index((kind, k)), d_model // 2

        def chunk(half, src):
            if only is None:
                return ysall.at[buf, src, pl.ds(half * per_exp, per_exp)]
            return ysall.at[buf, src, pl.ds(only * per_exp, per_exp), pl.ds(half * half_d, half_d)]

        def span(pairs):
            if only is None:
                return ysall.at[buf, pl.ds(0, pairs)]
            return ysall.at[buf, pl.ds(0, pairs), pl.ds(only * per_exp, per_exp)]

        return Exchange(me, n, chunk, span, ys_send.at[r], lambda group: ys_recv.at[r, group], (FIRST, SECOND, THIRD, MATE, MATE, MATE), r in DIRECT)

    def combine(r):
        kind, k, only = RINGS[r]
        buf = EXPERTS.index((kind, k))
        for b in range(batch) if only is None else (only,):
            at = pl.ds(b * toks, toks)
            got = ysall[buf, :, pl.ds(b * per_exp, per_exp), :].reshape(n * per_exp, d_model)
            yacc[at, :] += jnp.dot(cperm[buf, at, :], got, preferred_element_type=F32)

    def second_matmul(b):
        kind, k, only = job_of(b)
        live = pl.ds(0, 2 * rows if kind == "A" else rows if only is None else per_exp)
        out = jnp.dot(hidden[b % 2, live, :], w2buf[b % ahead], preferred_element_type=F32)
        if b % blocks:
            out = yexp[live, :] + out
        if (b + 1) % blocks:
            yexp[live, :] = out
            return
        buf = EXPERTS.index((kind, k))
        if only is None:
            ysall[buf, me] = out[:rows].astype(BF16)
        else:
            ysall[buf, me, pl.ds(only * per_exp, per_exp)] = out.astype(BF16)
        if kind == "A":
            yback[k] = out[rows:].astype(BF16)

    def run(firsts, seconds):
        for b in firsts:
            kind, k, only = job_of(b)
            if kind == "A" and b % blocks == 0:
                whole = xpair.at[k, pl.ds(rows, rows)]
                pltpu.make_async_remote_copy(src_ref=whole, dst_ref=whole, send_sem=xp_send.at[0], recv_sem=xp_recv.at[k], device_id={"data": pair}, device_id_type=MESH).wait_recv()
            w1_copy(b).wait()
        for b in seconds:
            w2_copy(b).wait()
        for b in sorted({*firsts, *(b + 1 for b in seconds)}):
            if b in firsts:
                kind, k, only = job_of(b)
                if kind == "A":
                    x_job = xpair[k]
                elif only is None:
                    x_job = xs[expert_of(kind, k)]
                else:
                    x_job = xs[expert_of(kind, k), pl.ds(only * per_exp, per_exp)]
                pre = jnp.dot(x_job, w1buf[b % ahead], preferred_element_type=F32)
            if b - 1 in seconds:
                second_matmul(b - 1)
            if b in firsts:
                hidden[b % 2, pl.ds(0, pre.shape[0]), :] = jax.nn.gelu(pre).astype(BF16)
        for b in firsts:
            if b + ahead < units:
                w1_copy(b + ahead).start()
        for b in seconds:
            if b + ahead < units:
                w2_copy(b + ahead).start()

    def act(kind, r):
        if kind == "S":
            pl.when(jnp.logical_not(upper))(tok1.second)
        elif kind == "L":
            tok1.arrived(MATE, 1)
            tok1.arrived(MATE_NEAR, 2)
            for src in (me, tok1.left, tok1.right):
                chip_logits(1, src)
        elif kind == "T":
            pl.when(jnp.logical_not(upper))(tok1.third)
        elif kind == "D":
            tok1.arrived(MATE_FAR, 1)
            chip_logits(1, tok1.far)
            dispatch(1)
        elif kind == "o":
            if RINGS[r][0] == "P":
                mine = yback.at[RINGS[r][1]]
                pltpu.make_async_remote_copy(src_ref=mine, dst_ref=mine, send_sem=yb_send.at[0], recv_sem=yb_recv.at[RINGS[r][1]], device_id={"data": pair}, device_id_type=MESH).wait_recv()
                ys_ex(r).start(4, 5)
            elif RINGS[r][0] == "A":
                y_to_pair(RINGS[r][1], 0, 1)
                ys_ex(r).start(0, 2)
                y_to_pair(RINGS[r][1], 2, 3)
                ys_ex(r).start(1, 3, 4, 5)
                y_to_pair(RINGS[r][1], 4, 5)
            else:
                ys_ex(r).own()
        elif kind == "f":
            ys_ex(r).first()
        elif kind == "s":
            ys_ex(r).second()
        elif kind == "t":
            ys_ex(r).third()
        else:
            ys_ex(r).arrived(MATE, 4)
            combine(r)

    firsts = seconds = 0
    for what in PROGRAM:
        kind, r = what[0], int(what[1:])
        with jax.named_scope(what if kind not in "BF" else f"{kind}{firsts}"):
            if kind == "B":
                run(range(firsts, firsts + r), range(seconds, firsts + r - 1))
                firsts, seconds = firsts + r, firsts + r - 1
            elif kind == "F":
                run((), (seconds,))
                seconds += 1
            else:
                act(kind, r)
    assert seconds == units

    with jax.named_scope("final"):
        for b in range(batch):
            at = pl.ds(b * toks, toks)
            pos = me * toks + lax.broadcasted_iota(jnp.int32, (toks, 1), 0)
            out_ref[b] = jnp.where(pos < len_ref[b], yacc[at, :] / qbuf[at, 0:1], 0.0).astype(BF16)
    with jax.named_scope("sent"):
        tok0.sent()
        tok1.sent()
        for r in range(len(RINGS)):
            ys_ex(r).sent(5 if RINGS[r][0] == "P" else 7)
        pltpu.make_async_remote_copy(src_ref=yback, dst_ref=yback, send_sem=xp_send.at[0], recv_sem=xp_recv.at[0], device_id={"data": pair}, device_id_type=MESH).wait_send()
        given = ysall.at[pl.ds(0, SHARED), pl.ds(0, 3)]
        pltpu.make_async_remote_copy(src_ref=given, dst_ref=given, send_sem=yb_send.at[0], recv_sem=yb_recv.at[0], device_id={"data": pair}, device_id_type=MESH).wait_send()


def solution(mesh):
    n = mesh.shape["seq"]

    def local_layer(tok_blk, len_blk, slot_param, logit_scale, w_in, w_out):
        batch, toks, d_model = tok_blk.shape
        n_slots = slot_param.shape[1]
        n_exp = w_in.shape[0]
        slot_loc = n_slots // n
        rows = batch * (slot_loc // n_exp)
        dma = pltpu.SemaphoreType.DMA
        any_spec = pl.BlockSpec(memory_space=pl.ANY)
        smem_spec = pl.BlockSpec(memory_space=pltpu.SMEM)
        return pl.pallas_call(
            functools.partial(kernel, n),
            out_shape=pltpu.VMEM(tok_blk.shape, BF16),
            in_specs=[any_spec, any_spec, any_spec, smem_spec, any_spec, any_spec],
            out_specs=pl.BlockSpec(memory_space=pltpu.VMEM),
            scratch_shapes=[
                pltpu.VMEM((batch, n, toks, d_model), BF16),
                pltpu.VMEM(slot_param.shape, BF16),
                pltpu.VMEM((slot_loc, d_model), BF16),
                pltpu.VMEM((batch, n // 2, slot_loc, 2 * toks), F32),
                pltpu.VMEM((batch * toks, n_slots), BF16),
                pltpu.VMEM((batch * toks, 128), F32),
                pltpu.VMEM((n_exp, batch * toks, n_slots // n_exp), BF16),
                pltpu.VMEM((n_exp, rows, d_model), BF16),
                pltpu.VMEM((SHARED, 2 * rows, d_model), BF16),
                pltpu.VMEM((n_exp, n, rows, d_model), BF16),
                pltpu.VMEM((SHARED, rows, d_model), BF16),
                pltpu.VMEM((2, 2 * rows, FF_BLOCK), BF16),
                pltpu.VMEM((2 * rows, d_model), F32),
                pltpu.VMEM((batch * toks, d_model), F32),
                pltpu.VMEM((AHEAD, d_model, FF_BLOCK), BF16),
                pltpu.VMEM((AHEAD, FF_BLOCK, d_model), BF16),
                dma((batch + 2,)), dma((AHEAD,)), dma((AHEAD,)),
                dma((batch,)), dma((batch, 6)), dma((len(RINGS),)), dma((len(RINGS), 4)),
                dma((1,)), dma((SHARED,)), dma((1,)), dma((SHARED,)),
                pltpu.SMEM((batch,), jnp.int32),
                pltpu.SemaphoreType.REGULAR,
            ],
            compiler_params=pltpu.CompilerParams(collective_id=0, has_side_effects=True, vmem_limit_bytes=VMEM_BYTES),
        )(tok_blk, len_blk, slot_param, logit_scale.reshape(1), w_in, w_out)

    return jax.shard_map(local_layer, mesh=mesh, in_specs=(P("data", "seq", None), P("data"), P(None, None), P(), P("seq", None, None), P("seq", None, None)), out_specs=P("data", "seq", None), check_vma=False)
```

```python
import functools

import jax
import jax.numpy as jnp
from jax import lax
from jax.experimental import pallas as pl
from jax.experimental.pallas import tpu as pltpu
from jax.sharding import PartitionSpec as P

EPSILON = 1e-6
NEG_FILL = -1e30
MESH = pl.DeviceIdType.MESH
F32 = jnp.float32
BF16 = jnp.bfloat16
FF_BLOCK = 1024
JOBS = (("U", 0, 0), ("U", 1, None), ("A", 0, None), ("A", 1, None), ("A", 2, None), ("U", 0, 1))
EXPERTS = (("U", 0), ("A", 0), ("A", 1), ("P", 0), ("A", 2), ("P", 1), ("U", 1), ("P", 2))
RINGS = (("U", 0, 0), ("U", 1, None), ("A", 0, None), ("A", 1, None), ("P", 0, None), ("A", 2, None), ("P", 1, None), ("U", 0, 1), ("P", 2, None))
BEFORE, SHARED = 1, 3
DIRECT = (0, 1, 7)
PROGRAM = (
    "B2", "S1", "L1", "B1", "T1", "D1", "B1", "B1", "o0", "B1", "B1", "B1", "F1", "o1", "B1", "B1", "B1", "f0", "s0", "B1", "B1", "o2",
    "t0", "f1", "B1", "B1", "B1", "F1", "o3", "s1", "t1", "m0", "B1", "B1", "f2", "f4", "B1", "m1", "B1", "s2", "s4", "B1", "o5", "B1",
    "B1", "B1", "f3", "f6", "F1", "o7", "s3", "s6", "t2", "o4", "t4", "f5", "f8", "s5", "s8", "t3", "o6", "m2", "t6", "f7", "s7", "o8",
    "m4", "t5", "t7", "t8", "m3", "m6", "m5", "m7", "m8",
)
AHEAD = 12
VMEM_BYTES = 62 * 1024 * 1024


def unit_rows(values):
    v32 = values.astype(F32)
    return (v32 * lax.rsqrt(jnp.sum(v32 * v32, axis=1, keepdims=True) + EPSILON)).astype(BF16)


FIRST, SECOND, THIRD, MATE, MATE_NEAR, MATE_FAR = range(6)


class Exchange:
    def __init__(self, me, n, chunk, span, send_sem, recv_sem, groups, direct=False):
        core = lax.rem(me, 2)
        self.me, self.mate = me, me + 1 - 2 * core
        self.right, self.left = lax.rem(me + 2, n), lax.rem(me + n - 2, n)
        self.far = lax.rem(me + n // 2, n)
        self.chunk, self.span, self.send_sem, self.recv_sem, self.groups, self.direct = chunk, span, send_sem, recv_sem, groups, direct

    def plan(self):
        me, right, left, far, mate = self.me, self.right, self.left, self.far, self.mate
        onward = [(0, me, far, THIRD), (1, me, far, THIRD)] if self.direct else [(0, left, right, THIRD), (1, right, left, THIRD)]
        return [(0, me, right, FIRST), (1, me, right, SECOND), (1, me, left, FIRST), (0, me, left, SECOND), (0, me, mate, MATE), (1, me, mate, MATE),
                *onward, (0, left, mate, MATE_NEAR), (1, right, mate, MATE_NEAR),
                (1, left, mate, MATE_NEAR), (0, right, mate, MATE_NEAR), (0, far, mate, MATE_FAR), (1, far, mate, MATE_FAR)]

    def start(self, *which):
        for half, src, to, group in (self.plan()[i] for i in which):
            ref = self.chunk(half, src)
            pltpu.make_async_remote_copy(src_ref=ref, dst_ref=ref, send_sem=self.send_sem, recv_sem=self.recv_sem(self.groups[group]), device_id={"seq": to}, device_id_type=MESH).start()

    def arrived(self, group, pairs):
        ref = self.span(pairs)
        pltpu.make_async_remote_copy(src_ref=ref, dst_ref=ref, send_sem=self.send_sem, recv_sem=self.recv_sem(group), device_id={"seq": self.mate}, device_id_type=MESH).wait_recv()

    def own(self):
        self.start(0, 1, 2, 3, 4, 5, *((6, 7) if self.direct else ()))

    def first(self):
        self.arrived(FIRST, 1)
        self.start(*(() if self.direct else (6, 7)), 8, 9)

    def second(self):
        self.arrived(SECOND, 1)
        self.start(10, 11)

    def third(self):
        self.arrived(THIRD, 1)
        self.start(12, 13)

    def sent(self):
        ref = self.span(7)
        pltpu.make_async_remote_copy(src_ref=ref, dst_ref=ref, send_sem=self.send_sem, recv_sem=self.recv_sem(0), device_id={"seq": self.mate}, device_id_type=MESH).wait_send()


def kernel(n, tok_hbm, len_hbm, phi_hbm, g_ref, w1_hbm, w2_hbm, out_ref, xall, phi, pnt, lt, cbuf, qbuf, cperm, xs, xpair, ysall, yback, hidden, yexp, yacc, w1buf, w2buf,
           loc_sem, w1_sem, w2_sem, tok_send, tok_recv, ys_send, ys_recv, xp_send, xp_recv, yb_send, yb_recv, len_ref, pairs_in):
    batch, _, toks, d_model = xall.shape
    n_exp, _, rows, _ = ysall.shape
    per_exp = rows // batch
    slot_loc = n_exp * per_exp
    blocks = w1_hbm.shape[2] // FF_BLOCK
    ahead = w1buf.shape[0]
    chips = n // 2
    me = lax.axis_index("seq")
    g = g_ref[0]

    data = lax.axis_index("data")
    odd = lax.rem(data, 2)
    pair = data + 1 - 2 * odd

    def expert_of(kind, k):
        if kind == "U":
            return k if k < BEFORE else k + 2 * SHARED
        return BEFORE + SHARED * (odd if kind == "A" else 1 - odd) + k

    units = len(JOBS) * blocks

    def job_of(b):
        return JOBS[b // blocks]

    def w1_copy(b):
        e, f0 = expert_of(*job_of(b)[:2]), b % blocks * FF_BLOCK
        return pltpu.make_async_copy(w1_hbm.at[e, :, pl.ds(f0, FF_BLOCK)], w1buf.at[b % ahead], w1_sem.at[b % ahead])

    def w2_copy(b):
        e, f0 = expert_of(*job_of(b)[:2]), b % blocks * FF_BLOCK
        return pltpu.make_async_copy(w2_hbm.at[e, pl.ds(f0, FF_BLOCK), :], w2buf.at[b % ahead], w2_sem.at[b % ahead])

    def x_to_pair(k, b):
        src, dst = pl.ds(b * per_exp, per_exp), pl.ds(rows + b * per_exp, per_exp)
        return pltpu.make_async_remote_copy(src_ref=xs.at[expert_of("P", k), src], dst_ref=xpair.at[k, dst], send_sem=xp_send.at[0], recv_sem=xp_recv.at[k], device_id={"data": pair}, device_id_type=MESH)

    def y_to_pair(k, *which):
        buf = EXPERTS.index(("P", k))
        r = RINGS.index(("P", k, None))
        plan = ((0, tok0.right, ys_recv.at[r, FIRST]), (1, tok0.left, ys_recv.at[r, FIRST]), (1, tok0.right, ys_recv.at[r, SECOND]), (0, tok0.left, ys_recv.at[r, SECOND]), (0, me, yb_recv.at[k]), (1, me, yb_recv.at[k]))
        for half, to, sem in (plan[i] for i in which):
            at = pl.ds(half * per_exp, per_exp)
            pltpu.make_async_remote_copy(src_ref=yback.at[k, at], dst_ref=ysall.at[buf, me, at], send_sem=yb_send.at[0], recv_sem=sem, device_id={"data": pair, "seq": to}, device_id_type=MESH).start()

    part = toks // 2
    tok0, tok1 = (Exchange(me, n, lambda half, src, b=b: xall.at[b, src, pl.ds(half * part, part)], lambda pairs, b=b: xall.at[b, pl.ds(0, pairs)], tok_send.at[b], lambda group, b=b: tok_recv.at[b, group], range(6)) for b in range(batch))
    barrier = pltpu.get_barrier_semaphore()
    for peer in (tok0.right, tok0.left, tok0.mate):
        pl.semaphore_signal(barrier, inc=1, device_id={"seq": peer}, device_id_type=MESH)
    pl.semaphore_signal(barrier, inc=1, device_id={"data": pair}, device_id_type=MESH)
    own_in = [pltpu.make_async_copy(tok_hbm.at[b], xall.at[b, me], loc_sem.at[b]) for b in range(batch)]
    for c in own_in:
        c.start()
    phi_in = pltpu.make_async_copy(phi_hbm, phi, loc_sem.at[batch])
    phi_in.start()
    len_in = pltpu.make_async_copy(len_hbm, len_ref, loc_sem.at[batch + 1])
    len_in.start()

    for c in own_in:
        c.wait()
    for u in range(min(ahead, units)):
        w1_copy(u).start()
        w2_copy(u).start()
    pl.semaphore_wait(barrier, 4)
    tok0.own()
    tok1.start(0, 2)
    for peer in (tok0.right, tok0.left):
        pl.semaphore_signal(pairs_in, inc=1, device_id={"seq": peer}, device_id_type=MESH)

    phi_in.wait()
    len_in.wait()
    d_rows = phi.shape[0]
    n_slots = phi.shape[1]
    step = 64

    def sum_sq(i, acc):
        v = phi[pl.ds(pl.multiple_of(i * step, step), step), :].astype(F32)
        return acc + jnp.sum((v * v).reshape(step // 8, 8, n_slots), axis=0)

    scale = lax.rsqrt(jnp.sum(lax.fori_loop(0, d_rows // step, sum_sq, jnp.zeros((8, n_slots), F32)), axis=0, keepdims=True) + EPSILON)

    def to_unit(i, _):
        at = pl.ds(pl.multiple_of(i * step, step), step)
        phi[at, :] = (phi[at, :].astype(F32) * scale).astype(BF16)
        return 0

    lax.fori_loop(0, d_rows // step, to_unit, 0)
    pnt[...] = phi[:, pl.ds(pl.multiple_of(me * slot_loc, slot_loc), slot_loc)].astype(F32).T.astype(BF16)

    for b in range(batch):
        logits = g * jnp.dot(unit_rows(xall[b, me]), phi[...], preferred_element_type=F32)
        comb = jnp.exp(logits - jnp.max(logits, axis=1, keepdims=True))
        at = pl.ds(b * toks, toks)
        qbuf[at, :] = jnp.broadcast_to(jnp.sum(comb, axis=1, keepdims=True), (toks, 128))
        cbuf[at, :] = comb.astype(BF16)

    tok0.first()
    tok1.start(1, 3, 4, 5)

    def regroup():
        j = lax.broadcasted_iota(jnp.int32, (n_slots, slot_loc), 0)
        k = lax.broadcasted_iota(jnp.int32, (n_slots, slot_loc), 1)
        first = j - ((k // per_exp) * slot_loc + lax.rem(k, per_exp))
        for r, what in enumerate(EXPERTS):
            pick = (first == expert_of(*what) * per_exp).astype(F32).astype(BF16)
            cperm[r] = jnp.dot(cbuf[...], pick, preferred_element_type=F32).astype(BF16)

    regroup()

    def chip_logits(b, src):
        chip = src // 2
        x_chip = xall[b, pl.ds(2 * chip, 2)].reshape(2 * toks, d_model)
        logits = g * lax.dot_general(pnt[...], unit_rows(x_chip), (((1,), (1,)), ((), ())), preferred_element_type=F32)
        pos = chip * (2 * toks) + lax.broadcasted_iota(jnp.int32, logits.shape, 1)
        lt[b, chip] = jnp.where(pos < len_ref[b], logits, NEG_FILL)

    def dispatch(b):
        parts = [lt[b, k] for k in range(chips)]
        top = jnp.max(functools.reduce(jnp.maximum, parts), axis=1, keepdims=True)
        disp = [jnp.exp(p - top) for p in parts]
        col_sum = jnp.sum(functools.reduce(jnp.add, disp), axis=1, keepdims=True)
        weights = jnp.concatenate([w.astype(BF16) for w in disp], axis=1)
        slot_sum = jnp.dot(weights, xall[b].reshape(n * toks, d_model), preferred_element_type=F32)
        at = pl.ds(b * per_exp, per_exp)
        xs[:, at, :] = (slot_sum / col_sum).astype(BF16).reshape(n_exp, per_exp, d_model)
        for k in range(SHARED):
            x_to_pair(k, b).start()
            xpair[k, at] = xs[expert_of("A", k), at]

    tok0.second()
    tok0.arrived(MATE, 1)
    chip_logits(0, me)
    tok1.first()
    tok0.arrived(MATE_NEAR, 2)
    chip_logits(0, tok0.left)
    chip_logits(0, tok0.right)
    tok0.third()
    upper = lax.rem(me, 2) == 1

    @pl.when(upper)
    def _():
        tok1.second()
        tok1.third()

    tok0.arrived(MATE_FAR, 1)
    chip_logits(0, tok0.far)
    dispatch(0)
    pl.semaphore_wait(pairs_in, 2)
    yacc[...] = jnp.zeros_like(yacc)

    def ys_ex(r):
        kind, k, only = RINGS[r]
        buf, half_d = EXPERTS.index((kind, k)), d_model // 2

        def chunk(half, src):
            if only is None:
                return ysall.at[buf, src, pl.ds(half * per_exp, per_exp)]
            return ysall.at[buf, src, pl.ds(only * per_exp, per_exp), pl.ds(half * half_d, half_d)]

        def span(pairs):
            if only is None:
                return ysall.at[buf, pl.ds(0, pairs)]
            return ysall.at[buf, pl.ds(0, pairs), pl.ds(only * per_exp, per_exp)]

        return Exchange(me, n, chunk, span, ys_send.at[0 if only is not None else 1 if kind == "P" else 2], lambda group: ys_recv.at[r, group], (FIRST, SECOND, THIRD, MATE, MATE, MATE), r in DIRECT)

    def combine(r):
        kind, k, only = RINGS[r]
        buf = EXPERTS.index((kind, k))
        for b in range(batch) if only is None else (only,):
            at = pl.ds(b * toks, toks)
            got = ysall[buf, :, pl.ds(b * per_exp, per_exp), :].reshape(n * per_exp, d_model)
            yacc[at, :] += jnp.dot(cperm[buf, at, :], got, preferred_element_type=F32)

    def second_matmul(b):
        kind, k, only = job_of(b)
        live = pl.ds(0, 2 * rows if kind == "A" else rows if only is None else per_exp)
        out = jnp.dot(hidden[b % 2, live, :], w2buf[b % ahead], preferred_element_type=F32)
        if b % blocks:
            out = yexp[live, :] + out
        if (b + 1) % blocks:
            yexp[live, :] = out
            return
        buf = EXPERTS.index((kind, k))
        if only is None:
            ysall[buf, me] = out[:rows].astype(BF16)
        else:
            ysall[buf, me, pl.ds(only * per_exp, per_exp)] = out.astype(BF16)
        if kind == "A":
            yback[k] = out[rows:].astype(BF16)

    def run(firsts, seconds):
        for b in firsts:
            kind, k, only = job_of(b)
            if kind == "A" and b % blocks == 0:
                whole = xpair.at[k, pl.ds(rows, rows)]
                pltpu.make_async_remote_copy(src_ref=whole, dst_ref=whole, send_sem=xp_send.at[0], recv_sem=xp_recv.at[k], device_id={"data": pair}, device_id_type=MESH).wait_recv()
            w1_copy(b).wait()
        for b in seconds:
            w2_copy(b).wait()
        for b in sorted({*firsts, *(b + 1 for b in seconds)}):
            if b in firsts:
                kind, k, only = job_of(b)
                if kind == "A":
                    x_job = xpair[k]
                elif only is None:
                    x_job = xs[expert_of(kind, k)]
                else:
                    x_job = xs[expert_of(kind, k), pl.ds(only * per_exp, per_exp)]
                pre = jnp.dot(x_job, w1buf[b % ahead], preferred_element_type=F32)
            if b - 1 in seconds:
                second_matmul(b - 1)
            if b in firsts:
                hidden[b % 2, pl.ds(0, pre.shape[0]), :] = jax.nn.gelu(pre).astype(BF16)
        for b in firsts:
            if b + ahead < units:
                w1_copy(b + ahead).start()
        for b in seconds:
            if b + ahead < units:
                w2_copy(b + ahead).start()

    def act(kind, r):
        if kind == "S":
            pl.when(jnp.logical_not(upper))(tok1.second)
        elif kind == "L":
            tok1.arrived(MATE, 1)
            tok1.arrived(MATE_NEAR, 2)
            for src in (me, tok1.left, tok1.right):
                chip_logits(1, src)
        elif kind == "T":
            pl.when(jnp.logical_not(upper))(tok1.third)
        elif kind == "D":
            tok1.arrived(MATE_FAR, 1)
            chip_logits(1, tok1.far)
            dispatch(1)
        elif kind == "o":
            if RINGS[r][0] == "P":
                mine = yback.at[RINGS[r][1]]
                pltpu.make_async_remote_copy(src_ref=mine, dst_ref=mine, send_sem=yb_send.at[0], recv_sem=yb_recv.at[RINGS[r][1]], device_id={"data": pair}, device_id_type=MESH).wait_recv()
                ys_ex(r).start(4, 5)
            elif RINGS[r][0] == "A":
                y_to_pair(RINGS[r][1], 0, 1)
                ys_ex(r).start(0, 2)
                y_to_pair(RINGS[r][1], 4, 5, 2, 3)
                ys_ex(r).start(1, 3, 4, 5)
            else:
                ys_ex(r).own()
        elif kind == "f":
            ys_ex(r).first()
        elif kind == "s":
            ys_ex(r).second()
        elif kind == "t":
            ys_ex(r).third()
        else:
            ys_ex(r).arrived(MATE, 4)
            combine(r)

    firsts = seconds = 0
    for what in PROGRAM:
        kind, r = what[0], int(what[1:])
        with jax.named_scope(what if kind not in "BF" else f"{kind}{firsts}"):
            if kind == "B":
                run(range(firsts, firsts + r), range(seconds, firsts + r - 1))
                firsts, seconds = firsts + r, firsts + r - 1
            elif kind == "F":
                run((), (seconds,))
                seconds += 1
            else:
                act(kind, r)
    assert seconds == units

    with jax.named_scope("final"):
        for b in range(batch):
            at = pl.ds(b * toks, toks)
            pos = me * toks + lax.broadcasted_iota(jnp.int32, (toks, 1), 0)
            out_ref[b] = jnp.where(pos < len_ref[b], yacc[at, :] / qbuf[at, 0:1], 0.0).astype(BF16)
    with jax.named_scope("sent"):
        tok0.sent()
        tok1.sent()
        halves = [ring for ring in RINGS if ring[2] is not None]
        sent_spans = (ysall.at[pl.ds(0, len(halves)), pl.ds(0, 7), pl.ds(0, per_exp)], ysall.at[pl.ds(0, SHARED), pl.ds(0, 5)], ysall.at[pl.ds(0, len(RINGS) - len(halves) - SHARED), pl.ds(0, 7)])
        for i, ref in enumerate(sent_spans):
            pltpu.make_async_remote_copy(src_ref=ref, dst_ref=ref, send_sem=ys_send.at[i], recv_sem=ys_recv.at[0, 0], device_id={"data": pair}, device_id_type=MESH).wait_send()
        pltpu.make_async_remote_copy(src_ref=yback, dst_ref=yback, send_sem=xp_send.at[0], recv_sem=xp_recv.at[0], device_id={"data": pair}, device_id_type=MESH).wait_send()
        given = ysall.at[pl.ds(0, SHARED), pl.ds(0, 3)]
        pltpu.make_async_remote_copy(src_ref=given, dst_ref=given, send_sem=yb_send.at[0], recv_sem=yb_recv.at[0], device_id={"data": pair}, device_id_type=MESH).wait_send()


def solution(mesh):
    n = mesh.shape["seq"]

    def local_layer(tok_blk, len_blk, slot_param, logit_scale, w_in, w_out):
        batch, toks, d_model = tok_blk.shape
        n_slots = slot_param.shape[1]
        n_exp = w_in.shape[0]
        slot_loc = n_slots // n
        rows = batch * (slot_loc // n_exp)
        dma = pltpu.SemaphoreType.DMA
        any_spec = pl.BlockSpec(memory_space=pl.ANY)
        smem_spec = pl.BlockSpec(memory_space=pltpu.SMEM)
        return pl.pallas_call(
            functools.partial(kernel, n),
            out_shape=pltpu.VMEM(tok_blk.shape, BF16),
            in_specs=[any_spec, any_spec, any_spec, smem_spec, any_spec, any_spec],
            out_specs=pl.BlockSpec(memory_space=pltpu.VMEM),
            scratch_shapes=[
                pltpu.VMEM((batch, n, toks, d_model), BF16),
                pltpu.VMEM(slot_param.shape, BF16),
                pltpu.VMEM((slot_loc, d_model), BF16),
                pltpu.VMEM((batch, n // 2, slot_loc, 2 * toks), F32),
                pltpu.VMEM((batch * toks, n_slots), BF16),
                pltpu.VMEM((batch * toks, 128), F32),
                pltpu.VMEM((n_exp, batch * toks, n_slots // n_exp), BF16),
                pltpu.VMEM((n_exp, rows, d_model), BF16),
                pltpu.VMEM((SHARED, 2 * rows, d_model), BF16),
                pltpu.VMEM((n_exp, n, rows, d_model), BF16),
                pltpu.VMEM((SHARED, rows, d_model), BF16),
                pltpu.VMEM((2, 2 * rows, FF_BLOCK), BF16),
                pltpu.VMEM((2 * rows, d_model), F32),
                pltpu.VMEM((batch * toks, d_model), F32),
                pltpu.VMEM((AHEAD, d_model, FF_BLOCK), BF16),
                pltpu.VMEM((AHEAD, FF_BLOCK, d_model), BF16),
                dma((batch + 2,)), dma((AHEAD,)), dma((AHEAD,)),
                dma((batch,)), dma((batch, 6)), dma((3,)), dma((len(RINGS), 4)),
                dma((1,)), dma((SHARED,)), dma((1,)), dma((SHARED,)),
                pltpu.SMEM((batch,), jnp.int32),
                pltpu.SemaphoreType.REGULAR,
            ],
            compiler_params=pltpu.CompilerParams(collective_id=0, has_side_effects=True, vmem_limit_bytes=VMEM_BYTES),
        )(tok_blk, len_blk, slot_param, logit_scale.reshape(1), w_in, w_out)

    return jax.shard_map(local_layer, mesh=mesh, in_specs=(P("data", "seq", None), P("data"), P(None, None), P(), P("seq", None, None), P("seq", None, None)), out_specs=P("data", "seq", None), check_vma=False)
```

```python
import functools

import jax
import jax.numpy as jnp
from jax import lax
from jax.experimental import pallas as pl
from jax.experimental.pallas import tpu as pltpu
from jax.sharding import PartitionSpec as P

EPSILON = 1e-6
NEG_FILL = -1e30
MESH = pl.DeviceIdType.MESH
F32 = jnp.float32
BF16 = jnp.bfloat16
FF_BLOCK = 1024
JOBS = (("U", 0, 0), ("U", 1, None), ("A", 0, None), ("A", 1, None), ("A", 2, None), ("U", 0, 1))
EXPERTS = (("U", 0), ("A", 0), ("A", 1), ("P", 0), ("A", 2), ("P", 1), ("U", 1), ("P", 2))
RINGS = (("U", 0, 0), ("U", 1, None), ("A", 0, None), ("A", 1, None), ("P", 0, None), ("A", 2, None), ("P", 1, None), ("U", 0, 1), ("P", 2, None))
BEFORE, SHARED = 1, 3
DIRECT = (0, 1, 7)
PROGRAM = (
    "B2", "S1", "L1", "B1", "T1", "D1", "B1", "B1", "o0", "B1", "B1", "B1", "B1", "o1", "B1", "B1", "f0", "s0", "B1", "B1", "o2", "t0",
    "f1", "B1", "B1", "G1", "o3", "s1", "t1", "m0", "B1", "B1", "f2", "f4", "B1", "m1", "B1", "s2", "s4", "B1", "o5", "B1", "B1", "B1",
    "f3", "f6", "F1", "o7", "s3", "s6", "t2", "o4", "t4", "f5", "f8", "s5", "s8", "t3", "o6", "m2", "t6", "f7", "s7", "o8", "m4", "t5",
    "t7", "t8", "m3", "m6", "m5", "m7", "m8",
)
AHEAD = 12
VMEM_BYTES = 62 * 1024 * 1024


def unit_rows(values):
    v32 = values.astype(F32)
    return (v32 * lax.rsqrt(jnp.sum(v32 * v32, axis=1, keepdims=True) + EPSILON)).astype(BF16)


FIRST, SECOND, THIRD, MATE, MATE_NEAR, MATE_FAR = range(6)


class Exchange:
    def __init__(self, me, n, chunk, span, send_sem, recv_sem, groups, direct=False):
        core = lax.rem(me, 2)
        self.me, self.mate = me, me + 1 - 2 * core
        self.right, self.left = lax.rem(me + 2, n), lax.rem(me + n - 2, n)
        self.far = lax.rem(me + n // 2, n)
        self.chunk, self.span, self.send_sem, self.recv_sem, self.groups, self.direct = chunk, span, send_sem, recv_sem, groups, direct

    def plan(self):
        me, right, left, far, mate = self.me, self.right, self.left, self.far, self.mate
        onward = [(0, me, far, THIRD), (1, me, far, THIRD)] if self.direct else [(0, left, right, THIRD), (1, right, left, THIRD)]
        return [(0, me, right, FIRST), (1, me, right, SECOND), (1, me, left, FIRST), (0, me, left, SECOND), (0, me, mate, MATE), (1, me, mate, MATE),
                *onward, (0, left, mate, MATE_NEAR), (1, right, mate, MATE_NEAR),
                (1, left, mate, MATE_NEAR), (0, right, mate, MATE_NEAR), (0, far, mate, MATE_FAR), (1, far, mate, MATE_FAR)]

    def start(self, *which):
        for half, src, to, group in (self.plan()[i] for i in which):
            ref = self.chunk(half, src)
            pltpu.make_async_remote_copy(src_ref=ref, dst_ref=ref, send_sem=self.send_sem, recv_sem=self.recv_sem(self.groups[group]), device_id={"seq": to}, device_id_type=MESH).start()

    def arrived(self, group, pairs):
        ref = self.span(pairs)
        pltpu.make_async_remote_copy(src_ref=ref, dst_ref=ref, send_sem=self.send_sem, recv_sem=self.recv_sem(group), device_id={"seq": self.mate}, device_id_type=MESH).wait_recv()

    def own(self):
        self.start(0, 1, 2, 3, 4, 5, *((6, 7) if self.direct else ()))

    def first(self):
        self.arrived(FIRST, 1)
        self.start(*(() if self.direct else (6, 7)), 8, 9)

    def second(self):
        self.arrived(SECOND, 1)
        self.start(10, 11)

    def third(self):
        self.arrived(THIRD, 1)
        self.start(12, 13)

    def sent(self):
        ref = self.span(7)
        pltpu.make_async_remote_copy(src_ref=ref, dst_ref=ref, send_sem=self.send_sem, recv_sem=self.recv_sem(0), device_id={"seq": self.mate}, device_id_type=MESH).wait_send()


def kernel(n, tok_hbm, len_hbm, phi_hbm, g_ref, w1_hbm, w2_hbm, out_ref, xall, phi, pnt, lt, cbuf, qbuf, cperm, xs, xpair, ysall, yback, hidden, yexp, yacc, w1buf, w2buf,
           loc_sem, w1_sem, w2_sem, tok_send, tok_recv, ys_send, ys_recv, xp_send, xp_recv, yb_send, yb_recv, len_ref, pairs_in):
    batch, _, toks, d_model = xall.shape
    n_exp, _, rows, _ = ysall.shape
    per_exp = rows // batch
    slot_loc = n_exp * per_exp
    blocks = w1_hbm.shape[2] // FF_BLOCK
    ahead = w1buf.shape[0]
    chips = n // 2
    me = lax.axis_index("seq")
    g = g_ref[0]

    data = lax.axis_index("data")
    odd = lax.rem(data, 2)
    pair = data + 1 - 2 * odd

    def expert_of(kind, k):
        if kind == "U":
            return k if k < BEFORE else k + 2 * SHARED
        return BEFORE + SHARED * (odd if kind == "A" else 1 - odd) + k

    units = len(JOBS) * blocks

    def job_of(b):
        return JOBS[b // blocks]

    def w1_copy(b):
        e, f0 = expert_of(*job_of(b)[:2]), b % blocks * FF_BLOCK
        return pltpu.make_async_copy(w1_hbm.at[e, :, pl.ds(f0, FF_BLOCK)], w1buf.at[b % ahead], w1_sem.at[b % ahead])

    def w2_copy(b):
        e, f0 = expert_of(*job_of(b)[:2]), b % blocks * FF_BLOCK
        return pltpu.make_async_copy(w2_hbm.at[e, pl.ds(f0, FF_BLOCK), :], w2buf.at[b % ahead], w2_sem.at[b % ahead])

    def x_to_pair(k, b):
        src, dst = pl.ds(b * per_exp, per_exp), pl.ds(rows + b * per_exp, per_exp)
        return pltpu.make_async_remote_copy(src_ref=xs.at[expert_of("P", k), src], dst_ref=xpair.at[k, dst], send_sem=xp_send.at[0], recv_sem=xp_recv.at[k], device_id={"data": pair}, device_id_type=MESH)

    def y_to_pair(k, *which):
        buf = EXPERTS.index(("P", k))
        r = RINGS.index(("P", k, None))
        plan = ((0, tok0.right, ys_recv.at[r, FIRST]), (1, tok0.left, ys_recv.at[r, FIRST]), (1, tok0.right, ys_recv.at[r, SECOND]), (0, tok0.left, ys_recv.at[r, SECOND]), (0, me, yb_recv.at[k]), (1, me, yb_recv.at[k]))
        for half, to, sem in (plan[i] for i in which):
            at = pl.ds(half * per_exp, per_exp)
            pltpu.make_async_remote_copy(src_ref=yback.at[k, at], dst_ref=ysall.at[buf, me, at], send_sem=yb_send.at[0], recv_sem=sem, device_id={"data": pair, "seq": to}, device_id_type=MESH).start()

    part = toks // 2
    tok0, tok1 = (Exchange(me, n, lambda half, src, b=b: xall.at[b, src, pl.ds(half * part, part)], lambda pairs, b=b: xall.at[b, pl.ds(0, pairs)], tok_send.at[b], lambda group, b=b: tok_recv.at[b, group], range(6)) for b in range(batch))
    barrier = pltpu.get_barrier_semaphore()
    for peer in (tok0.right, tok0.left, tok0.mate):
        pl.semaphore_signal(barrier, inc=1, device_id={"seq": peer}, device_id_type=MESH)
    pl.semaphore_signal(barrier, inc=1, device_id={"data": pair}, device_id_type=MESH)
    own_in = [pltpu.make_async_copy(tok_hbm.at[b], xall.at[b, me], loc_sem.at[b]) for b in range(batch)]
    for c in own_in:
        c.start()
    phi_in = pltpu.make_async_copy(phi_hbm, phi, loc_sem.at[batch])
    phi_in.start()
    len_in = pltpu.make_async_copy(len_hbm, len_ref, loc_sem.at[batch + 1])
    len_in.start()

    for c in own_in:
        c.wait()
    for u in range(min(ahead, units)):
        w1_copy(u).start()
        w2_copy(u).start()
    pl.semaphore_wait(barrier, 4)
    tok0.own()
    tok1.start(0, 2)
    for peer in (tok0.right, tok0.left):
        pl.semaphore_signal(pairs_in, inc=1, device_id={"seq": peer}, device_id_type=MESH)

    phi_in.wait()
    len_in.wait()
    d_rows = phi.shape[0]
    n_slots = phi.shape[1]
    step = 64

    def sum_sq(i, acc):
        v = phi[pl.ds(pl.multiple_of(i * step, step), step), :].astype(F32)
        return acc + jnp.sum((v * v).reshape(step // 8, 8, n_slots), axis=0)

    scale = lax.rsqrt(jnp.sum(lax.fori_loop(0, d_rows // step, sum_sq, jnp.zeros((8, n_slots), F32)), axis=0, keepdims=True) + EPSILON)

    def to_unit(i, _):
        at = pl.ds(pl.multiple_of(i * step, step), step)
        phi[at, :] = (phi[at, :].astype(F32) * scale).astype(BF16)
        return 0

    lax.fori_loop(0, d_rows // step, to_unit, 0)
    pnt[...] = phi[:, pl.ds(pl.multiple_of(me * slot_loc, slot_loc), slot_loc)].astype(F32).T.astype(BF16)

    for b in range(batch):
        logits = g * jnp.dot(unit_rows(xall[b, me]), phi[...], preferred_element_type=F32)
        comb = jnp.exp(logits - jnp.max(logits, axis=1, keepdims=True))
        at = pl.ds(b * toks, toks)
        qbuf[at, :] = jnp.broadcast_to(jnp.sum(comb, axis=1, keepdims=True), (toks, 128))
        cbuf[at, :] = comb.astype(BF16)

    tok0.first()
    tok1.start(1, 3, 4, 5)

    def regroup():
        j = lax.broadcasted_iota(jnp.int32, (n_slots, slot_loc), 0)
        k = lax.broadcasted_iota(jnp.int32, (n_slots, slot_loc), 1)
        first = j - ((k // per_exp) * slot_loc + lax.rem(k, per_exp))
        for r, what in enumerate(EXPERTS):
            pick = (first == expert_of(*what) * per_exp).astype(F32).astype(BF16)
            cperm[r] = jnp.dot(cbuf[...], pick, preferred_element_type=F32).astype(BF16)

    regroup()

    def chip_logits(b, src):
        chip = src // 2
        x_chip = xall[b, pl.ds(2 * chip, 2)].reshape(2 * toks, d_model)
        logits = g * lax.dot_general(pnt[...], unit_rows(x_chip), (((1,), (1,)), ((), ())), preferred_element_type=F32)
        pos = chip * (2 * toks) + lax.broadcasted_iota(jnp.int32, logits.shape, 1)
        lt[b, chip] = jnp.where(pos < len_ref[b], logits, NEG_FILL)

    def dispatch(b):
        parts = [lt[b, k] for k in range(chips)]
        top = jnp.max(functools.reduce(jnp.maximum, parts), axis=1, keepdims=True)
        disp = [jnp.exp(p - top) for p in parts]
        col_sum = jnp.sum(functools.reduce(jnp.add, disp), axis=1, keepdims=True)
        weights = jnp.concatenate([w.astype(BF16) for w in disp], axis=1)
        slot_sum = jnp.dot(weights, xall[b].reshape(n * toks, d_model), preferred_element_type=F32)
        at = pl.ds(b * per_exp, per_exp)
        xs[:, at, :] = (slot_sum / col_sum).astype(BF16).reshape(n_exp, per_exp, d_model)
        for k in range(SHARED):
            x_to_pair(k, b).start()
            xpair[k, at] = xs[expert_of("A", k), at]

    tok0.second()
    tok0.arrived(MATE, 1)
    chip_logits(0, me)
    tok1.first()
    tok0.arrived(MATE_NEAR, 2)
    chip_logits(0, tok0.left)
    chip_logits(0, tok0.right)
    tok0.third()
    upper = lax.rem(me, 2) == 1

    @pl.when(upper)
    def _():
        tok1.second()
        tok1.third()

    tok0.arrived(MATE_FAR, 1)
    chip_logits(0, tok0.far)
    dispatch(0)
    pl.semaphore_wait(pairs_in, 2)
    yacc[...] = jnp.zeros_like(yacc)

    def ys_ex(r):
        kind, k, only = RINGS[r]
        buf, half_d = EXPERTS.index((kind, k)), d_model // 2

        def chunk(half, src):
            if only is None:
                return ysall.at[buf, src, pl.ds(half * per_exp, per_exp)]
            return ysall.at[buf, src, pl.ds(only * per_exp, per_exp), pl.ds(half * half_d, half_d)]

        def span(pairs):
            if only is None:
                return ysall.at[buf, pl.ds(0, pairs)]
            return ysall.at[buf, pl.ds(0, pairs), pl.ds(only * per_exp, per_exp)]

        return Exchange(me, n, chunk, span, ys_send.at[0 if only is not None else 1 if kind == "P" else 2], lambda group: ys_recv.at[r, group], (FIRST, SECOND, THIRD, MATE, MATE, MATE), r in DIRECT)

    def combine(r):
        kind, k, only = RINGS[r]
        buf = EXPERTS.index((kind, k))
        for b in range(batch) if only is None else (only,):
            at = pl.ds(b * toks, toks)
            got = ysall[buf, :, pl.ds(b * per_exp, per_exp), :].reshape(n * per_exp, d_model)
            yacc[at, :] += jnp.dot(cperm[buf, at, :], got, preferred_element_type=F32)

    def second_matmul(b):
        kind, k, only = job_of(b)
        live = pl.ds(0, 2 * rows if kind == "A" else rows if only is None else per_exp)
        out = jnp.dot(hidden[b % 2, live, :], w2buf[b % ahead], preferred_element_type=F32)
        if b % blocks:
            out = yexp[live, :] + out
        if (b + 1) % blocks:
            yexp[live, :] = out
            return
        buf = EXPERTS.index((kind, k))
        if only is None:
            ysall[buf, me] = out[:rows].astype(BF16)
        else:
            ysall[buf, me, pl.ds(only * per_exp, per_exp)] = out.astype(BF16)
        if kind == "A":
            yback[k] = out[rows:].astype(BF16)

    def run(firsts, seconds):
        for b in firsts:
            kind, k, only = job_of(b)
            if kind == "A" and b % blocks == 0:
                whole = xpair.at[k, pl.ds(rows, rows)]
                pltpu.make_async_remote_copy(src_ref=whole, dst_ref=whole, send_sem=xp_send.at[0], recv_sem=xp_recv.at[k], device_id={"data": pair}, device_id_type=MESH).wait_recv()
            w1_copy(b).wait()
        for b in seconds:
            w2_copy(b).wait()
        for b in sorted({*firsts, *(b + 1 for b in seconds)}):
            if b in firsts:
                kind, k, only = job_of(b)
                if kind == "A":
                    x_job = xpair[k]
                elif only is None:
                    x_job = xs[expert_of(kind, k)]
                else:
                    x_job = xs[expert_of(kind, k), pl.ds(only * per_exp, per_exp)]
                pre = jnp.dot(x_job, w1buf[b % ahead], preferred_element_type=F32)
            if b - 1 in seconds:
                second_matmul(b - 1)
            if b in firsts:
                hidden[b % 2, pl.ds(0, pre.shape[0]), :] = jax.nn.gelu(pre).astype(BF16)
        for b in firsts:
            if b + ahead < units:
                w1_copy(b + ahead).start()
        for b in seconds:
            if b + ahead < units:
                w2_copy(b + ahead).start()

    def act(kind, r):
        if kind == "S":
            pl.when(jnp.logical_not(upper))(tok1.second)
        elif kind == "L":
            tok1.arrived(MATE, 1)
            tok1.arrived(MATE_NEAR, 2)
            for src in (me, tok1.left, tok1.right):
                chip_logits(1, src)
        elif kind == "T":
            pl.when(jnp.logical_not(upper))(tok1.third)
        elif kind == "D":
            tok1.arrived(MATE_FAR, 1)
            chip_logits(1, tok1.far)
            dispatch(1)
        elif kind == "o":
            if RINGS[r][0] == "P":
                mine = yback.at[RINGS[r][1]]
                pltpu.make_async_remote_copy(src_ref=mine, dst_ref=mine, send_sem=yb_send.at[0], recv_sem=yb_recv.at[RINGS[r][1]], device_id={"data": pair}, device_id_type=MESH).wait_recv()
                ys_ex(r).start(4, 5)
            elif RINGS[r][0] == "A":
                y_to_pair(RINGS[r][1], 0, 1)
                ys_ex(r).start(0, 2)
                y_to_pair(RINGS[r][1], 4, 5, 2, 3)
                ys_ex(r).start(1, 3, 4, 5)
            else:
                ys_ex(r).own()
        elif kind == "f":
            ys_ex(r).first()
        elif kind == "s":
            ys_ex(r).second()
        elif kind == "t":
            ys_ex(r).third()
        else:
            ys_ex(r).arrived(MATE, 4)
            combine(r)

    firsts = seconds = 0
    for what in PROGRAM:
        kind, r = what[0], int(what[1:])
        with jax.named_scope(what if kind not in "BFG" else f"{kind}{firsts}"):
            if kind == "B":
                run(range(firsts, firsts + r), range(seconds, firsts + r - 1))
                firsts, seconds = firsts + r, firsts + r - 1
            elif kind == "F":
                run((), (seconds,))
                seconds += 1
            elif kind == "G":
                run(range(firsts, firsts + r), range(seconds, firsts + r))
                firsts = seconds = firsts + r
            else:
                act(kind, r)
    assert seconds == units

    with jax.named_scope("final"):
        for b in range(batch):
            at = pl.ds(b * toks, toks)
            pos = me * toks + lax.broadcasted_iota(jnp.int32, (toks, 1), 0)
            out_ref[b] = jnp.where(pos < len_ref[b], yacc[at, :] / qbuf[at, 0:1], 0.0).astype(BF16)
    with jax.named_scope("sent"):
        tok0.sent()
        tok1.sent()
        halves = [ring for ring in RINGS if ring[2] is not None]
        sent_spans = (ysall.at[pl.ds(0, len(halves)), pl.ds(0, 7), pl.ds(0, per_exp)], ysall.at[pl.ds(0, SHARED), pl.ds(0, 5)], ysall.at[pl.ds(0, len(RINGS) - len(halves) - SHARED), pl.ds(0, 7)])
        for i, ref in enumerate(sent_spans):
            pltpu.make_async_remote_copy(src_ref=ref, dst_ref=ref, send_sem=ys_send.at[i], recv_sem=ys_recv.at[0, 0], device_id={"data": pair}, device_id_type=MESH).wait_send()
        pltpu.make_async_remote_copy(src_ref=yback, dst_ref=yback, send_sem=xp_send.at[0], recv_sem=xp_recv.at[0], device_id={"data": pair}, device_id_type=MESH).wait_send()
        given = ysall.at[pl.ds(0, SHARED), pl.ds(0, 3)]
        pltpu.make_async_remote_copy(src_ref=given, dst_ref=given, send_sem=yb_send.at[0], recv_sem=yb_recv.at[0], device_id={"data": pair}, device_id_type=MESH).wait_send()


def solution(mesh):
    n = mesh.shape["seq"]

    def local_layer(tok_blk, len_blk, slot_param, logit_scale, w_in, w_out):
        batch, toks, d_model = tok_blk.shape
        n_slots = slot_param.shape[1]
        n_exp = w_in.shape[0]
        slot_loc = n_slots // n
        rows = batch * (slot_loc // n_exp)
        dma = pltpu.SemaphoreType.DMA
        any_spec = pl.BlockSpec(memory_space=pl.ANY)
        smem_spec = pl.BlockSpec(memory_space=pltpu.SMEM)
        return pl.pallas_call(
            functools.partial(kernel, n),
            out_shape=pltpu.VMEM(tok_blk.shape, BF16),
            in_specs=[any_spec, any_spec, any_spec, smem_spec, any_spec, any_spec],
            out_specs=pl.BlockSpec(memory_space=pltpu.VMEM),
            scratch_shapes=[
                pltpu.VMEM((batch, n, toks, d_model), BF16),
                pltpu.VMEM(slot_param.shape, BF16),
                pltpu.VMEM((slot_loc, d_model), BF16),
                pltpu.VMEM((batch, n // 2, slot_loc, 2 * toks), F32),
                pltpu.VMEM((batch * toks, n_slots), BF16),
                pltpu.VMEM((batch * toks, 128), F32),
                pltpu.VMEM((n_exp, batch * toks, n_slots // n_exp), BF16),
                pltpu.VMEM((n_exp, rows, d_model), BF16),
                pltpu.VMEM((SHARED, 2 * rows, d_model), BF16),
                pltpu.VMEM((n_exp, n, rows, d_model), BF16),
                pltpu.VMEM((SHARED, rows, d_model), BF16),
                pltpu.VMEM((2, 2 * rows, FF_BLOCK), BF16),
                pltpu.VMEM((2 * rows, d_model), F32),
                pltpu.VMEM((batch * toks, d_model), F32),
                pltpu.VMEM((AHEAD, d_model, FF_BLOCK), BF16),
                pltpu.VMEM((AHEAD, FF_BLOCK, d_model), BF16),
                dma((batch + 2,)), dma((AHEAD,)), dma((AHEAD,)),
                dma((batch,)), dma((batch, 6)), dma((3,)), dma((len(RINGS), 4)),
                dma((1,)), dma((SHARED,)), dma((1,)), dma((SHARED,)),
                pltpu.SMEM((batch,), jnp.int32),
                pltpu.SemaphoreType.REGULAR,
            ],
            compiler_params=pltpu.CompilerParams(collective_id=0, has_side_effects=True, vmem_limit_bytes=VMEM_BYTES),
        )(tok_blk, len_blk, slot_param, logit_scale.reshape(1), w_in, w_out)

    return jax.shard_map(local_layer, mesh=mesh, in_specs=(P("data", "seq", None), P("data"), P(None, None), P(), P("seq", None, None), P("seq", None, None)), out_specs=P("data", "seq", None), check_vma=False)
```

```python
import functools

import jax
import jax.numpy as jnp
from jax import lax
from jax.experimental import pallas as pl
from jax.experimental.pallas import tpu as pltpu
from jax.sharding import PartitionSpec as P

EPSILON = 1e-6
NEG_FILL = -1e30
MESH = pl.DeviceIdType.MESH
F32 = jnp.float32
BF16 = jnp.bfloat16
FF_BLOCK = 1024
JOBS = (("U", 0, 0), ("U", 1, None), ("A", 0, None), ("A", 1, None), ("A", 2, None), ("U", 0, 1))
EXPERTS = (("U", 0), ("A", 0), ("A", 1), ("P", 0), ("A", 2), ("P", 1), ("U", 1), ("P", 2))
RINGS = (("U", 0, 0), ("U", 1, None), ("A", 0, None), ("A", 1, None), ("P", 0, None), ("A", 2, None), ("P", 1, None), ("U", 0, 1), ("P", 2, None))
BEFORE, SHARED = 1, 3
DIRECT = (0, 1, 7)
PROGRAM = (
    "B2", "S1", "L1", "B1", "T1", "D1", "B1", "B1", "o0", "B1", "B1", "B1", "B1", "o1", "B1", "B1", "f0", "s0", "B1", "B1", "o2", "t0",
    "f1", "B1", "B1", "G1", "o3", "s1", "t1", "m0", "B1", "B1", "f2", "f4", "B1", "m1", "B1", "s2", "s4", "B1", "o5", "B1", "B1", "B1",
    "f3", "f6", "F1", "o7", "s3", "s6", "t2", "o4", "t4", "f5", "f8", "s5", "s8", "t3", "o6", "m2", "t6", "f7", "s7", "o8", "m4", "t5",
    "t7", "t8", "m3", "m6", "m5", "m7", "m8",
)
AHEAD = 12
VMEM_BYTES = 62 * 1024 * 1024


def unit_rows(values):
    v32 = values.astype(F32)
    return (v32 * lax.rsqrt(jnp.sum(v32 * v32, axis=1, keepdims=True) + EPSILON)).astype(BF16)


FIRST, SECOND, THIRD, MATE, MATE_NEAR, MATE_FAR = range(6)


class Exchange:
    def __init__(self, me, n, chunk, span, send_sem, recv_sem, groups, direct=False):
        core = lax.rem(me, 2)
        self.me, self.mate = me, me + 1 - 2 * core
        self.right, self.left = lax.rem(me + 2, n), lax.rem(me + n - 2, n)
        self.far = lax.rem(me + n // 2, n)
        self.chunk, self.span, self.send_sem, self.recv_sem, self.groups, self.direct = chunk, span, send_sem, recv_sem, groups, direct

    def plan(self):
        me, right, left, far, mate = self.me, self.right, self.left, self.far, self.mate
        onward = [(0, me, far, THIRD), (1, me, far, THIRD)] if self.direct else [(0, left, right, THIRD), (1, right, left, THIRD)]
        return [(0, me, right, FIRST), (1, me, right, SECOND), (1, me, left, FIRST), (0, me, left, SECOND), (0, me, mate, MATE), (1, me, mate, MATE),
                *onward, (0, left, mate, MATE_NEAR), (1, right, mate, MATE_NEAR),
                (1, left, mate, MATE_NEAR), (0, right, mate, MATE_NEAR), (0, far, mate, MATE_FAR), (1, far, mate, MATE_FAR)]

    def start(self, *which):
        for half, src, to, group in (self.plan()[i] for i in which):
            ref = self.chunk(half, src)
            pltpu.make_async_remote_copy(src_ref=ref, dst_ref=ref, send_sem=self.send_sem, recv_sem=self.recv_sem(self.groups[group]), device_id={"seq": to}, device_id_type=MESH).start()

    def arrived(self, group, pairs):
        ref = self.span(pairs)
        pltpu.make_async_remote_copy(src_ref=ref, dst_ref=ref, send_sem=self.send_sem, recv_sem=self.recv_sem(group), device_id={"seq": self.mate}, device_id_type=MESH).wait_recv()

    def own(self):
        self.start(0, 1, 2, 3, 4, 5, *((6, 7) if self.direct else ()))

    def first(self):
        self.arrived(FIRST, 1)
        self.start(*(() if self.direct else (6, 7)), 8, 9)

    def second(self):
        self.arrived(SECOND, 1)
        self.start(10, 11)

    def third(self):
        self.arrived(THIRD, 1)
        self.start(12, 13)

    def sent(self):
        ref = self.span(7)
        pltpu.make_async_remote_copy(src_ref=ref, dst_ref=ref, send_sem=self.send_sem, recv_sem=self.recv_sem(0), device_id={"seq": self.mate}, device_id_type=MESH).wait_send()


def kernel(n, tok_hbm, len_hbm, phi_hbm, g_ref, w1_hbm, w2_hbm, out_ref, xall, phi, pnt, lt, cbuf, qbuf, cperm, xs, xpair, ysall, yback, hidden, yexp, yacc, w1buf, w2buf,
           loc_sem, w_sem, tok_send, tok_recv, ys_send, ys_recv, xp_send, xp_recv, yb_send, yb_recv, len_ref, pairs_in):
    batch, _, toks, d_model = xall.shape
    n_exp, _, rows, _ = ysall.shape
    per_exp = rows // batch
    slot_loc = n_exp * per_exp
    blocks = w1_hbm.shape[2] // FF_BLOCK
    ahead = w1buf.shape[0]
    chips = n // 2
    me = lax.axis_index("seq")
    g = g_ref[0]

    data = lax.axis_index("data")
    odd = lax.rem(data, 2)
    pair = data + 1 - 2 * odd

    def expert_of(kind, k):
        if kind == "U":
            return k if k < BEFORE else k + 2 * SHARED
        return BEFORE + SHARED * (odd if kind == "A" else 1 - odd) + k

    units = len(JOBS) * blocks

    def job_of(b):
        return JOBS[b // blocks]

    def w1_copy(b):
        e, f0 = expert_of(*job_of(b)[:2]), b % blocks * FF_BLOCK
        return pltpu.make_async_copy(w1_hbm.at[e, :, pl.ds(f0, FF_BLOCK)], w1buf.at[b % ahead], w_sem.at[b % ahead])

    def w2_copy(b):
        e, f0 = expert_of(*job_of(b)[:2]), b % blocks * FF_BLOCK
        return pltpu.make_async_copy(w2_hbm.at[e, pl.ds(f0, FF_BLOCK), :], w2buf.at[b % ahead], w_sem.at[b % ahead])

    def x_to_pair(k, b):
        src, dst = pl.ds(b * per_exp, per_exp), pl.ds(rows + b * per_exp, per_exp)
        return pltpu.make_async_remote_copy(src_ref=xs.at[expert_of("P", k), src], dst_ref=xpair.at[k, dst], send_sem=xp_send.at[0], recv_sem=xp_recv.at[k], device_id={"data": pair}, device_id_type=MESH)

    def y_to_pair(k, *which):
        buf = EXPERTS.index(("P", k))
        r = RINGS.index(("P", k, None))
        plan = ((0, tok0.right, ys_recv.at[r, FIRST]), (1, tok0.left, ys_recv.at[r, FIRST]), (1, tok0.right, ys_recv.at[r, SECOND]), (0, tok0.left, ys_recv.at[r, SECOND]), (0, me, yb_recv.at[k]), (1, me, yb_recv.at[k]))
        for half, to, sem in (plan[i] for i in which):
            at = pl.ds(half * per_exp, per_exp)
            pltpu.make_async_remote_copy(src_ref=yback.at[k, at], dst_ref=ysall.at[buf, me, at], send_sem=yb_send.at[0], recv_sem=sem, device_id={"data": pair, "seq": to}, device_id_type=MESH).start()

    part = toks // 2
    tok0, tok1 = (Exchange(me, n, lambda half, src, b=b: xall.at[b, src, pl.ds(half * part, part)], lambda pairs, b=b: xall.at[b, pl.ds(0, pairs)], tok_send.at[b], lambda group, b=b: tok_recv.at[b, group], range(6)) for b in range(batch))
    barrier = pltpu.get_barrier_semaphore()
    for peer in (tok0.right, tok0.left, tok0.mate):
        pl.semaphore_signal(barrier, inc=1, device_id={"seq": peer}, device_id_type=MESH)
    pl.semaphore_signal(barrier, inc=1, device_id={"data": pair}, device_id_type=MESH)
    own_in = [pltpu.make_async_copy(tok_hbm.at[b], xall.at[b, me], loc_sem.at[b]) for b in range(batch)]
    for c in own_in:
        c.start()
    phi_in = pltpu.make_async_copy(phi_hbm, phi, loc_sem.at[batch])
    phi_in.start()
    len_in = pltpu.make_async_copy(len_hbm, len_ref, loc_sem.at[batch + 1])
    len_in.start()

    for c in own_in:
        c.wait()
    for u in range(min(ahead, units)):
        w1_copy(u).start()
        w2_copy(u).start()
    pl.semaphore_wait(barrier, 4)
    tok0.own()
    tok1.start(0, 2)
    for peer in (tok0.right, tok0.left):
        pl.semaphore_signal(pairs_in, inc=1, device_id={"seq": peer}, device_id_type=MESH)

    phi_in.wait()
    len_in.wait()
    d_rows = phi.shape[0]
    n_slots = phi.shape[1]
    step = 64

    def sum_sq(i, acc):
        v = phi[pl.ds(pl.multiple_of(i * step, step), step), :].astype(F32)
        return acc + jnp.sum((v * v).reshape(step // 8, 8, n_slots), axis=0)

    scale = lax.rsqrt(jnp.sum(lax.fori_loop(0, d_rows // step, sum_sq, jnp.zeros((8, n_slots), F32)), axis=0, keepdims=True) + EPSILON)

    def to_unit(i, _):
        at = pl.ds(pl.multiple_of(i * step, step), step)
        phi[at, :] = (phi[at, :].astype(F32) * scale).astype(BF16)
        return 0

    lax.fori_loop(0, d_rows // step, to_unit, 0)
    pnt[...] = phi[:, pl.ds(pl.multiple_of(me * slot_loc, slot_loc), slot_loc)].astype(F32).T.astype(BF16)

    for b in range(batch):
        logits = g * jnp.dot(unit_rows(xall[b, me]), phi[...], preferred_element_type=F32)
        comb = jnp.exp(logits - jnp.max(logits, axis=1, keepdims=True))
        at = pl.ds(b * toks, toks)
        qbuf[at, :] = jnp.broadcast_to(jnp.sum(comb, axis=1, keepdims=True), (toks, 128))
        cbuf[at, :] = comb.astype(BF16)

    tok0.first()
    tok1.start(1, 3, 4, 5)

    def regroup():
        j = lax.broadcasted_iota(jnp.int32, (n_slots, slot_loc), 0)
        k = lax.broadcasted_iota(jnp.int32, (n_slots, slot_loc), 1)
        first = j - ((k // per_exp) * slot_loc + lax.rem(k, per_exp))
        for r, what in enumerate(EXPERTS):
            pick = (first == expert_of(*what) * per_exp).astype(F32).astype(BF16)
            cperm[r] = jnp.dot(cbuf[...], pick, preferred_element_type=F32).astype(BF16)

    regroup()

    def chip_logits(b, src):
        chip = src // 2
        x_chip = xall[b, pl.ds(2 * chip, 2)].reshape(2 * toks, d_model)
        logits = g * lax.dot_general(pnt[...], unit_rows(x_chip), (((1,), (1,)), ((), ())), preferred_element_type=F32)
        pos = chip * (2 * toks) + lax.broadcasted_iota(jnp.int32, logits.shape, 1)
        lt[b, chip] = jnp.where(pos < len_ref[b], logits, NEG_FILL)

    def dispatch(b):
        parts = [lt[b, k] for k in range(chips)]
        top = jnp.max(functools.reduce(jnp.maximum, parts), axis=1, keepdims=True)
        disp = [jnp.exp(p - top) for p in parts]
        col_sum = jnp.sum(functools.reduce(jnp.add, disp), axis=1, keepdims=True)
        weights = jnp.concatenate([w.astype(BF16) for w in disp], axis=1)
        slot_sum = jnp.dot(weights, xall[b].reshape(n * toks, d_model), preferred_element_type=F32)
        at = pl.ds(b * per_exp, per_exp)
        xs[:, at, :] = (slot_sum / col_sum).astype(BF16).reshape(n_exp, per_exp, d_model)
        for k in range(SHARED):
            x_to_pair(k, b).start()
            xpair[k, at] = xs[expert_of("A", k), at]

    tok0.second()
    tok0.arrived(MATE, 1)
    chip_logits(0, me)
    tok1.first()
    tok0.arrived(MATE_NEAR, 2)
    chip_logits(0, tok0.left)
    chip_logits(0, tok0.right)
    tok0.third()
    upper = lax.rem(me, 2) == 1

    @pl.when(upper)
    def _():
        tok1.second()
        tok1.third()

    tok0.arrived(MATE_FAR, 1)
    chip_logits(0, tok0.far)
    dispatch(0)
    pl.semaphore_wait(pairs_in, 2)
    yacc[...] = jnp.zeros_like(yacc)

    def ys_ex(r):
        kind, k, only = RINGS[r]
        buf, half_d = EXPERTS.index((kind, k)), d_model // 2

        def chunk(half, src):
            if only is None:
                return ysall.at[buf, src, pl.ds(half * per_exp, per_exp)]
            return ysall.at[buf, src, pl.ds(only * per_exp, per_exp), pl.ds(half * half_d, half_d)]

        def span(pairs):
            if only is None:
                return ysall.at[buf, pl.ds(0, pairs)]
            return ysall.at[buf, pl.ds(0, pairs), pl.ds(only * per_exp, per_exp)]

        return Exchange(me, n, chunk, span, ys_send.at[0 if only is not None else 1 if kind == "P" else 2], lambda group: ys_recv.at[r, group], (FIRST, SECOND, THIRD, MATE, MATE, MATE), r in DIRECT)

    def combine(r):
        kind, k, only = RINGS[r]
        buf = EXPERTS.index((kind, k))
        for b in range(batch) if only is None else (only,):
            at = pl.ds(b * toks, toks)
            got = ysall[buf, :, pl.ds(b * per_exp, per_exp), :].reshape(n * per_exp, d_model)
            yacc[at, :] += jnp.dot(cperm[buf, at, :], got, preferred_element_type=F32)

    def second_matmul(b):
        kind, k, only = job_of(b)
        live = pl.ds(0, 2 * rows if kind == "A" else rows if only is None else per_exp)
        out = jnp.dot(hidden[b % 2, live, :], w2buf[b % ahead], preferred_element_type=F32)
        if b % blocks:
            out = yexp[live, :] + out
        if (b + 1) % blocks:
            yexp[live, :] = out
            return
        buf = EXPERTS.index((kind, k))
        if only is None:
            ysall[buf, me] = out[:rows].astype(BF16)
        else:
            ysall[buf, me, pl.ds(only * per_exp, per_exp)] = out.astype(BF16)
        if kind == "A":
            yback[k] = out[rows:].astype(BF16)

    def run(firsts, seconds):
        for b in firsts:
            kind, k, only = job_of(b)
            if kind == "A" and b % blocks == 0:
                whole = xpair.at[k, pl.ds(rows, rows)]
                pltpu.make_async_remote_copy(src_ref=whole, dst_ref=whole, send_sem=xp_send.at[0], recv_sem=xp_recv.at[k], device_id={"data": pair}, device_id_type=MESH).wait_recv()
            both = w1buf.at[pl.ds(0, 2)]
            pltpu.make_async_copy(both, both, w_sem.at[b % ahead]).wait()
        for b in sorted({*firsts, *(b + 1 for b in seconds)}):
            if b in firsts:
                kind, k, only = job_of(b)
                if kind == "A":
                    x_job = xpair[k]
                elif only is None:
                    x_job = xs[expert_of(kind, k)]
                else:
                    x_job = xs[expert_of(kind, k), pl.ds(only * per_exp, per_exp)]
                pre = jnp.dot(x_job, w1buf[b % ahead], preferred_element_type=F32)
            if b - 1 in seconds:
                second_matmul(b - 1)
            if b in firsts:
                hidden[b % 2, pl.ds(0, pre.shape[0]), :] = jax.nn.gelu(pre).astype(BF16)
        for b in firsts:
            if b + ahead < units:
                w1_copy(b + ahead).start()
        for b in seconds:
            if b + ahead < units:
                w2_copy(b + ahead).start()

    def act(kind, r):
        if kind == "S":
            pl.when(jnp.logical_not(upper))(tok1.second)
        elif kind == "L":
            tok1.arrived(MATE, 1)
            tok1.arrived(MATE_NEAR, 2)
            for src in (me, tok1.left, tok1.right):
                chip_logits(1, src)
        elif kind == "T":
            pl.when(jnp.logical_not(upper))(tok1.third)
        elif kind == "D":
            tok1.arrived(MATE_FAR, 1)
            chip_logits(1, tok1.far)
            dispatch(1)
        elif kind == "o":
            if RINGS[r][0] == "P":
                mine = yback.at[RINGS[r][1]]
                pltpu.make_async_remote_copy(src_ref=mine, dst_ref=mine, send_sem=yb_send.at[0], recv_sem=yb_recv.at[RINGS[r][1]], device_id={"data": pair}, device_id_type=MESH).wait_recv()
                ys_ex(r).start(4, 5)
            elif RINGS[r][0] == "A":
                y_to_pair(RINGS[r][1], 0, 1)
                ys_ex(r).start(0, 2)
                y_to_pair(RINGS[r][1], 4, 5, 2, 3)
                ys_ex(r).start(1, 3, 4, 5)
            else:
                ys_ex(r).own()
        elif kind == "f":
            ys_ex(r).first()
        elif kind == "s":
            ys_ex(r).second()
        elif kind == "t":
            ys_ex(r).third()
        else:
            ys_ex(r).arrived(MATE, 4)
            combine(r)

    firsts = seconds = 0
    for what in PROGRAM:
        kind, r = what[0], int(what[1:])
        with jax.named_scope(what if kind not in "BFG" else f"{kind}{firsts}"):
            if kind == "B":
                run(range(firsts, firsts + r), range(seconds, firsts + r - 1))
                firsts, seconds = firsts + r, firsts + r - 1
            elif kind == "F":
                run((), (seconds,))
                seconds += 1
            elif kind == "G":
                run(range(firsts, firsts + r), range(seconds, firsts + r))
                firsts = seconds = firsts + r
            else:
                act(kind, r)
    assert seconds == units

    with jax.named_scope("final"):
        for b in range(batch):
            at = pl.ds(b * toks, toks)
            pos = me * toks + lax.broadcasted_iota(jnp.int32, (toks, 1), 0)
            out_ref[b] = jnp.where(pos < len_ref[b], yacc[at, :] / qbuf[at, 0:1], 0.0).astype(BF16)
    with jax.named_scope("sent"):
        tok0.sent()
        tok1.sent()
        halves = [ring for ring in RINGS if ring[2] is not None]
        sent_spans = (ysall.at[pl.ds(0, len(halves)), pl.ds(0, 7), pl.ds(0, per_exp)], ysall.at[pl.ds(0, SHARED), pl.ds(0, 5)], ysall.at[pl.ds(0, len(RINGS) - len(halves) - SHARED), pl.ds(0, 7)])
        for i, ref in enumerate(sent_spans):
            pltpu.make_async_remote_copy(src_ref=ref, dst_ref=ref, send_sem=ys_send.at[i], recv_sem=ys_recv.at[0, 0], device_id={"data": pair}, device_id_type=MESH).wait_send()
        pltpu.make_async_remote_copy(src_ref=yback, dst_ref=yback, send_sem=xp_send.at[0], recv_sem=xp_recv.at[0], device_id={"data": pair}, device_id_type=MESH).wait_send()
        given = ysall.at[pl.ds(0, SHARED), pl.ds(0, 3)]
        pltpu.make_async_remote_copy(src_ref=given, dst_ref=given, send_sem=yb_send.at[0], recv_sem=yb_recv.at[0], device_id={"data": pair}, device_id_type=MESH).wait_send()


def solution(mesh):
    n = mesh.shape["seq"]

    def local_layer(tok_blk, len_blk, slot_param, logit_scale, w_in, w_out):
        batch, toks, d_model = tok_blk.shape
        n_slots = slot_param.shape[1]
        n_exp = w_in.shape[0]
        slot_loc = n_slots // n
        rows = batch * (slot_loc // n_exp)
        dma = pltpu.SemaphoreType.DMA
        any_spec = pl.BlockSpec(memory_space=pl.ANY)
        smem_spec = pl.BlockSpec(memory_space=pltpu.SMEM)
        return pl.pallas_call(
            functools.partial(kernel, n),
            out_shape=pltpu.VMEM(tok_blk.shape, BF16),
            in_specs=[any_spec, any_spec, any_spec, smem_spec, any_spec, any_spec],
            out_specs=pl.BlockSpec(memory_space=pltpu.VMEM),
            scratch_shapes=[
                pltpu.VMEM((batch, n, toks, d_model), BF16),
                pltpu.VMEM(slot_param.shape, BF16),
                pltpu.VMEM((slot_loc, d_model), BF16),
                pltpu.VMEM((batch, n // 2, slot_loc, 2 * toks), F32),
                pltpu.VMEM((batch * toks, n_slots), BF16),
                pltpu.VMEM((batch * toks, 128), F32),
                pltpu.VMEM((n_exp, batch * toks, n_slots // n_exp), BF16),
                pltpu.VMEM((n_exp, rows, d_model), BF16),
                pltpu.VMEM((SHARED, 2 * rows, d_model), BF16),
                pltpu.VMEM((n_exp, n, rows, d_model), BF16),
                pltpu.VMEM((SHARED, rows, d_model), BF16),
                pltpu.VMEM((2, 2 * rows, FF_BLOCK), BF16),
                pltpu.VMEM((2 * rows, d_model), F32),
                pltpu.VMEM((batch * toks, d_model), F32),
                pltpu.VMEM((AHEAD, d_model, FF_BLOCK), BF16),
                pltpu.VMEM((AHEAD, FF_BLOCK, d_model), BF16),
                dma((batch + 2,)), dma((AHEAD,)),
                dma((batch,)), dma((batch, 6)), dma((3,)), dma((len(RINGS), 4)),
                dma((1,)), dma((SHARED,)), dma((1,)), dma((SHARED,)),
                pltpu.SMEM((batch,), jnp.int32),
                pltpu.SemaphoreType.REGULAR,
            ],
            compiler_params=pltpu.CompilerParams(collective_id=0, has_side_effects=True, vmem_limit_bytes=VMEM_BYTES),
        )(tok_blk, len_blk, slot_param, logit_scale.reshape(1), w_in, w_out)

    return jax.shard_map(local_layer, mesh=mesh, in_specs=(P("data", "seq", None), P("data"), P(None, None), P(), P("seq", None, None), P("seq", None, None)), out_specs=P("data", "seq", None), check_vma=False)
```
